32 devices in a mesh: lat: 4 (over y, x), lon: 8 (over z, core).
Axes of the slice: x: 2, y: 2, z: 4, core: 2. Of those that a mesh axis runs over, the one named last changes fastest.
Arguments:
- block_input: float32 [96, 192, 384], P('lat', 'lon'), may hold values from -90 to 90, as said below
- cotangent: float32 [96, 192, 384], P('lat', 'lon'), may hold values from -6 to 6
- weights: float32 [1769472], replicated, may hold values from -4 to 4, as said below
- first_moment: float32 [1769472], P(('lat', 'lon')), may hold values from -3 to 3
- second_moment: float32 [1769472], P(('lat', 'lon')), may hold values from 0.05 to 2
- bias_table: float32 [12, 529], replicated, may hold values from -5 to 5
- bias_index: int32 [144, 144], replicated, may hold values from 0 to 528
- region_ids: int32 [96, 192], P('lat', 'lon'), may hold values from 0 to 2
Outputs:
- grad_input: float32 [96, 192, 384], P('lat', 'lon')
- weights_new: float32 [1769472], replicated
- first_new: float32 [1769472], P(('lat', 'lon'))
- second_new: float32 [1769472], P(('lat', 'lon'))
- table_grad: float32 [12, 529], replicated
The draws below stay inside these ranges and needn't reach their ends.
Inputs may be any that keep to these rules, and one draw needn't show every extreme that they name: `block_input`: Tokens' features; real values. `weights`: real values. `region_ids`: entry (r, c) is the region of the token at ((r + 6) mod 96, (c + 6) mod 192) of the input grid.
All inputs are finite; a program needn't handle non-finite values.
Results may differ from the reference program's by a relative error of at most 0.0003.
Values sent between devices are 32-bit elements; how exact they have to be, the bound alone decides.
A program may use at most 128 MiB of HBM per device.

```python
import math
import jax
import jax.numpy as jnp
from jax import lax

D = 384
HEADS = 12
FF = 1536
WIN = 12
HEAD_DIM = 32
SHIFT = 6
BIAS = 529
NPARAM = 1769472
LAT = 96
LON = 192
TOKENS = 18432


def draw_block_input(key, part):
    streams = jax.random.split(jax.random.fold_in(key, 7), 1)
    sample = jax.random.normal(streams[0], (LAT, LON, D), jnp.float32)
    return jnp.clip(sample, -90.0, 90.0)


def draw_weights(key, part):
    streams = jax.random.split(jax.random.fold_in(key, 13), 6)
    query = jax.random.normal(streams[0], (D, D), jnp.float32) * D ** (-0.5)
    keyed = jax.random.normal(streams[1], (D, D), jnp.float32) * D ** (-0.5)
    valued = jax.random.normal(streams[2], (D, D), jnp.float32) * D ** (-0.5)
    w_proj = jax.random.normal(streams[3], (D, D), jnp.float32) * D ** (-0.5)
    w_up = jax.random.normal(streams[4], (D, FF), jnp.float32) * D ** (-0.5)
    w_down = jax.random.normal(streams[5], (FF, D), jnp.float32) * FF ** (-0.5)
    w_qkv = jnp.concatenate([query, keyed, valued], axis=1)
    packed = jnp.concatenate([w_qkv.reshape(-1), w_proj.reshape(-1), w_up.reshape(-1), w_down.reshape(-1)])
    return jnp.clip(packed, -4.0, 4.0)


def place_ends(drawn, own_key, smallest, largest):
    extent = drawn.shape
    index_at = [jax.random.randint(jax.random.fold_in(own_key, axis), (), 0, extent[axis]) for axis in range(len(extent))]
    drawn = drawn.at[tuple(index_at)].set(smallest)
    longest = extent.index(max(extent))
    index_at[longest] = (index_at[longest] + 1) % extent[longest]
    return drawn.at[tuple(index_at)].set(largest)


def levels(own_key, extent, shards, smallest, largest):
    gain = 1.0
    for axis_at, parts in shards:
        heights = jax.random.uniform(jax.random.fold_in(jax.random.fold_in(own_key, 6), axis_at), (parts,), jnp.float32, smallest / len(shards), largest / len(shards))
        gain = gain * jnp.repeat(jnp.exp(heights), extent[axis_at] // parts).reshape((-1,) + (1,) * (len(extent) - 1 - axis_at))
    return gain


def bell_draw(key, extent, scale, limit, cuts=(), dtype=jnp.bfloat16):
    gain = levels(key, extent, cuts, -0.22, 0.18) if cuts else 1.0
    values = jax.random.normal(key, extent, jnp.float32) * scale * gain
    return jnp.minimum(jnp.maximum(values, -limit), limit).astype(dtype)


def setup_inputs(seed: int = 0) -> dict:
    arg_keys = jax.random.split(jax.random.key(seed), 9)
    block_input = draw_block_input(jax.random.fold_in(arg_keys[8], 71), 0)
    cotangent = bell_draw(arg_keys[1], (LAT, LON, D), 1.0, 6.0, ((0, 4), (1, 8)), jnp.float32)
    weights = draw_weights(jax.random.fold_in(arg_keys[8], 71), 0)
    first_moment = bell_draw(arg_keys[3], (NPARAM,), 0.5, 3.0, ((0, 32),), jnp.float32)
    second_moment = jnp.clip(jnp.exp(math.log(2.0) - 3.6888794 * jax.random.uniform(arg_keys[4], (NPARAM,), jnp.float32) ** levels(arg_keys[4], (NPARAM,), ((0, 32),), -0.2, 0.2)), 0.05, 2.0)
    bias_table = bell_draw(arg_keys[5], (HEADS, BIAS), 1.0, 5.0, (), jnp.float32)
    bias_index = place_ends(jax.random.randint(arg_keys[6], (WIN * WIN, WIN * WIN), 0, BIAS), jax.random.fold_in(arg_keys[6], 1), 0, BIAS - 1).astype(jnp.int32)
    region_ids = place_ends(jax.random.randint(arg_keys[7], (LAT, LON), 0, 3), jax.random.fold_in(arg_keys[7], 1), 0, 2).astype(jnp.int32)
    return dict(block_input=block_input, cotangent=cotangent, weights=weights, first_moment=first_moment, second_moment=second_moment, bias_table=bias_table, bias_index=bias_index, region_ids=region_ids)


precise = lax.Precision.HIGHEST

def normalize(values):
    center = values - lax.optimization_barrier(jnp.mean(values, axis=-1, keepdims=True))
    spread = lax.optimization_barrier(jnp.mean(center * center, axis=-1, keepdims=True))
    return center / jnp.sqrt(spread + 1e-05)

def windows(tensor):
    height, breadth, features = tensor.shape
    blocks = tensor.reshape(height // WIN, WIN, breadth // WIN, WIN, features)
    return blocks.transpose(0, 2, 1, 3, 4).reshape(-1, WIN * WIN, features)

def unwindow(blocks, height, breadth):
    features = blocks.shape[-1]
    tensor = blocks.reshape(height // WIN, breadth // WIN, WIN, WIN, features)
    return tensor.transpose(0, 2, 1, 3, 4).reshape(height, breadth, features)

def unpack(packed):
    first_cut = D * 3 * D
    second_cut = first_cut + D * D
    third_cut = second_cut + D * FF
    return (packed[:first_cut].reshape(D, 3 * D), packed[first_cut:second_cut].reshape(D, D), packed[second_cut:third_cut].reshape(D, FF), packed[third_cut:].reshape(FF, D))

def attend(tensor, w_all, bias_table, bias_index, region_ids, wrapped):
    w_qkv, w_proj, _, _ = unpack(w_all)
    height, breadth, _ = tensor.shape
    flat_rows = normalize(tensor).reshape(-1, D)
    mixed = jnp.dot(flat_rows, w_qkv, precision=precise, preferred_element_type=jnp.float32)
    mixed = windows(mixed.reshape(height, breadth, 3 * D))
    window_count = mixed.shape[0]
    query = mixed[:, :, :D].reshape(window_count, WIN * WIN, HEADS, HEAD_DIM)
    keyed = mixed[:, :, D:2 * D].reshape(window_count, WIN * WIN, HEADS, HEAD_DIM)
    valued = mixed[:, :, 2 * D:].reshape(window_count, WIN * WIN, HEADS, HEAD_DIM)
    scores = jnp.einsum('wihd,wjhd->whij', query, keyed, precision=precise) / math.sqrt(HEAD_DIM)
    scores = scores + jnp.take(bias_table, bias_index, axis=1)[None]
    labels = windows(region_ids[:, :, None])[:, :, 0]
    halves = windows(jnp.broadcast_to(wrapped[:, None, None], (height, breadth, 1)).astype(jnp.int32))[:, :, 0]
    allowed = (labels[:, :, None] == labels[:, None, :]) & (halves[:, :, None] == halves[:, None, :])
    allowed = allowed[:, None]
    masked = jnp.where(allowed, scores, -jnp.inf)
    summit = lax.stop_gradient(lax.optimization_barrier(jnp.max(masked, axis=-1, keepdims=True)))
    raised = jnp.exp(masked - summit)
    probability = raised / lax.optimization_barrier(jnp.sum(raised, axis=-1, keepdims=True))
    context = jnp.einsum('whij,wjhd->wihd', probability, valued, precision=precise)
    context = unwindow(context.reshape(window_count, WIN * WIN, D), height, breadth).reshape(-1, D)
    return jnp.dot(context, w_proj, precision=precise, preferred_element_type=jnp.float32).reshape(height, breadth, D)

def feed(tensor, w_all):
    _, _, w_up, w_down = unpack(w_all)
    flat_rows = normalize(tensor).reshape(-1, D)
    hidden = jax.nn.gelu(jnp.dot(flat_rows, w_up, precision=precise, preferred_element_type=jnp.float32), approximate=True)
    return jnp.dot(hidden, w_down, precision=precise, preferred_element_type=jnp.float32).reshape(tensor.shape)

def reference(block_input, cotangent, weights, first_moment, second_moment, bias_table, bias_index, region_ids):
    wrapped = jnp.arange(LAT) >= LAT - SHIFT

    def forward(tensor, w_all, table):
        moved = jnp.roll(tensor, (-SHIFT, -SHIFT), (0, 1))
        mixed = moved + attend(moved, w_all, table, bias_index, region_ids, wrapped)
        output = mixed + feed(mixed, w_all)
        return jnp.roll(output, (SHIFT, SHIFT), (0, 1))
    _, pullback = jax.vjp(forward, block_input, weights, bias_table)
    grad_input, grad_weights, grad_table = pullback(cotangent)
    factor = 1.0 / math.sqrt(TOKENS)
    grad_weights = grad_weights * factor
    first_new = 0.9 * first_moment + 0.1 * grad_weights
    second_new = 0.95 * second_moment + 0.05 * grad_weights * grad_weights
    weights_new = weights - 0.01 * first_new / (jnp.sqrt(second_new) + 1e-08)
    return (grad_input, weights_new, first_new, second_new, grad_table * factor)
```

```python
import functools
import math

import jax
import jax.numpy as jnp
from jax import lax
from jax.experimental import pallas as pl
from jax.experimental.pallas import tpu as pltpu
from jax.sharding import PartitionSpec as P

D = 384
HEADS = 12
FF = 1536
WIN = 12
HEAD_DIM = 32
SHIFT = 6
TOK = WIN * WIN
LOW = 32
HEAD_ROWS = 16
LANES = 128
CHUNKS = 4

high = lax.Precision.HIGH
F32 = jnp.float32
BF16 = jnp.bfloat16
NN = (((1,), (0,)), ((), ()))
NT = (((1,), (1,)), ((), ()))
TN = (((0,), (0,)), ((), ()))


def passed_along(value, axis, by):
    size = lax.axis_size(axis)
    return lax.ppermute(value, axis, [(i, (i + by) % size) for i in range(size)])


def windows(tensor):
    height, breadth, features = tensor.shape
    blocks = tensor.reshape(height // WIN, WIN, breadth // WIN, WIN, features)
    return blocks.transpose(0, 2, 1, 3, 4).reshape(-1, WIN * WIN, features)


def unwindow(blocks, height, breadth):
    features = blocks.shape[-1]
    tensor = blocks.reshape(height // WIN, breadth // WIN, WIN, WIN, features)
    return tensor.transpose(0, 2, 1, 3, 4).reshape(height, breadth, features)


def unpack(packed):
    first_cut = D * 3 * D
    second_cut = first_cut + D * D
    third_cut = second_cut + D * FF
    return (
        packed[:first_cut].reshape(D, 3 * D),
        packed[first_cut:second_cut].reshape(D, D),
        packed[second_cut:third_cut].reshape(D, FF),
        packed[third_cut:].reshape(FF, D),
    )


def split(value):
    upper = value.astype(BF16)
    return upper, (value - upper.astype(F32)).astype(BF16)


def mul(a, b, dims):
    return lax.dot_general(a, b, dims, preferred_element_type=F32)


def dot3(a, b, dims):
    return mul(a[0], b[0], dims) + mul(a[0], b[1], dims) + mul(a[1], b[0], dims)


def head_of(pair, h):
    at = h * HEAD_DIM
    return pair[0][:, at : at + HEAD_DIM], pair[1][:, at : at + HEAD_DIM]


def attention_forward_kernel(qkv_ref, bias_ref, row_ref, col_ref, context_ref, prob_ref):
    q = split(qkv_ref[0, :, :D] * (1.0 / math.sqrt(HEAD_DIM)))
    k = split(qkv_ref[0, :, D : 2 * D])
    v = split(qkv_ref[0, :, 2 * D :])
    allowed = col_ref[0] == row_ref[0]
    parts = []
    for h in range(HEADS):
        scores = dot3(head_of(q, h), head_of(k, h), NT) + bias_ref[h]
        masked = jnp.where(allowed, scores, -jnp.inf)
        raised = jnp.exp(masked - jnp.max(masked, axis=-1, keepdims=True))
        prob = raised / jnp.sum(raised, axis=-1, keepdims=True)
        prob_ref[0, h] = prob
        parts.append(dot3(split(prob), head_of(v, h), NN))
    context_ref[0] = jnp.concatenate(parts, axis=1)


def attention_backward_kernel(qkv_ref, prob_ref, grad_ref, dqkv_ref, dbias_ref):
    @pl.when(pl.program_id(0) == 0)
    def _():
        dbias_ref[...] = jnp.zeros_like(dbias_ref)

    scale = 1.0 / math.sqrt(HEAD_DIM)
    q = split(qkv_ref[0, :, :D])
    k = split(qkv_ref[0, :, D : 2 * D])
    v = split(qkv_ref[0, :, 2 * D :])
    g = split(grad_ref[0])
    dq, dk, dv = [], [], []
    for h in range(HEADS):
        prob = prob_ref[0, h]
        g_h = head_of(g, h)
        dv.append(dot3(split(prob), g_h, TN))
        dprob = dot3(g_h, head_of(v, h), NT)
        dscore = prob * (dprob - jnp.sum(prob * dprob, axis=-1, keepdims=True))
        dbias_ref[h] += dscore
        dscore = split(dscore * scale)
        dq.append(dot3(dscore, head_of(k, h), NN))
        dk.append(dot3(dscore, head_of(q, h), TN))
    dqkv_ref[0] = jnp.concatenate(dq + dk + dv, axis=1)


def bias_kernel(levels, table_ref, index_ref, bias_ref):
    upper, lower = split(table_ref[...])
    rows = lax.broadcasted_iota(jnp.int32, (LOW, TOK), 0)
    for r in range(index_ref.shape[0]):
        index = index_ref[r : r + 1, :]
        low = index & (LOW - 1)
        high_part = index >> 5
        hot = jnp.where(rows == low, 1.0, 0.0).astype(BF16)
        spread = mul(upper, hot, NN) + mul(lower, hot, NN)
        total = jnp.zeros((HEAD_ROWS, TOK), F32)
        for level in range(levels):
            total = jnp.where(
                high_part == level, spread[level * HEAD_ROWS : (level + 1) * HEAD_ROWS], total
            )
        bias_ref[:, r, :] = total[:HEADS]


def table_kernel(levels, grad_ref, index_ref, table_ref):
    @pl.when(pl.program_id(0) == 0)
    def _():
        table_ref[...] = jnp.zeros_like(table_ref)

    rows = lax.broadcasted_iota(jnp.int32, (LOW, TOK), 0)
    for r in range(index_ref.shape[0]):
        index = index_ref[r : r + 1, :]
        low = index & (LOW - 1)
        high_part = index >> 5
        hot = jnp.where(rows == low, 1.0, 0.0).astype(BF16)
        grad = jnp.concatenate(
            [grad_ref[:, r, :], jnp.zeros((HEAD_ROWS - HEADS, TOK), F32)], axis=0
        )
        stacked = jnp.concatenate(
            [jnp.where(high_part == level, grad, 0.0) for level in range(levels)], axis=0
        )
        upper, lower = split(stacked)
        table_ref[...] += mul(upper, hot, NT) + mul(lower, hot, NT)


def attention_forward(qkv, bias, row_label, col_label):
    count = qkv.shape[0]
    return pl.pallas_call(
        attention_forward_kernel,
        grid=(count,),
        in_specs=[
            pl.BlockSpec((1, TOK, 3 * D), lambda w: (w, 0, 0)),
            pl.BlockSpec((HEADS, TOK, TOK), lambda w: (0, 0, 0)),
            pl.BlockSpec((1, 1, TOK), lambda w: (w, 0, 0)),
            pl.BlockSpec((1, TOK, 1), lambda w: (w, 0, 0)),
        ],
        out_specs=(
            pl.BlockSpec((1, TOK, D), lambda w: (w, 0, 0)),
            pl.BlockSpec((1, HEADS, TOK, TOK), lambda w: (w, 0, 0, 0)),
        ),
        out_shape=(
            jax.ShapeDtypeStruct((count, TOK, D), F32),
            jax.ShapeDtypeStruct((count, HEADS, TOK, TOK), F32),
        ),
        cost_estimate=pl.CostEstimate(
            flops=40000000 * count, bytes_accessed=4000000 * count, transcendentals=250000 * count
        ),
    )(qkv, bias, row_label, col_label)


def attention_backward(qkv, prob, grad):
    count = qkv.shape[0]
    return pl.pallas_call(
        attention_backward_kernel,
        grid=(count,),
        in_specs=[
            pl.BlockSpec((1, TOK, 3 * D), lambda w: (w, 0, 0)),
            pl.BlockSpec((1, HEADS, TOK, TOK), lambda w: (w, 0, 0, 0)),
            pl.BlockSpec((1, TOK, D), lambda w: (w, 0, 0)),
        ],
        out_specs=(
            pl.BlockSpec((1, TOK, 3 * D), lambda w: (w, 0, 0)),
            pl.BlockSpec((HEADS, TOK, TOK), lambda w: (0, 0, 0)),
        ),
        out_shape=(
            jax.ShapeDtypeStruct((count, TOK, 3 * D), F32),
            jax.ShapeDtypeStruct((HEADS, TOK, TOK), F32),
        ),
        cost_estimate=pl.CostEstimate(
            flops=80000000 * count, bytes_accessed=4000000 * count, transcendentals=0
        ),
    )(qkv, prob, grad)


def look_up(table, index):
    entries = table.shape[1]
    levels = -(-entries // LOW)
    padded = jnp.pad(table, ((0, HEAD_ROWS - HEADS), (0, levels * LOW - entries)))
    padded = padded.reshape(HEAD_ROWS, levels, LOW).transpose(1, 0, 2).reshape(-1, LOW)
    return pl.pallas_call(
        functools.partial(bias_kernel, levels),
        grid=(TOK // 8,),
        in_specs=[
            pl.BlockSpec((levels * HEAD_ROWS, LOW), lambda i: (0, 0)),
            pl.BlockSpec((8, TOK), lambda i: (i, 0)),
        ],
        out_specs=pl.BlockSpec((HEADS, 8, TOK), lambda i: (0, i, 0)),
        out_shape=jax.ShapeDtypeStruct((HEADS, TOK, TOK), F32),
        cost_estimate=pl.CostEstimate(flops=1000000000, bytes_accessed=2000000, transcendentals=0),
    )(padded, index)


def table_gradient(grad, index, entries):
    levels = -(-entries // LOW)
    stacked = pl.pallas_call(
        functools.partial(table_kernel, levels),
        grid=(TOK // 8,),
        in_specs=[
            pl.BlockSpec((HEADS, 8, TOK), lambda i: (0, i, 0)),
            pl.BlockSpec((8, TOK), lambda i: (i, 0)),
        ],
        out_specs=pl.BlockSpec((levels * HEAD_ROWS, LOW), lambda i: (0, 0)),
        out_shape=jax.ShapeDtypeStruct((levels * HEAD_ROWS, LOW), F32),
        cost_estimate=pl.CostEstimate(flops=1000000000, bytes_accessed=2000000, transcendentals=0),
    )(grad, index)
    return stacked


def unstack_table(stacked, entries):
    levels = -(-entries // LOW)
    table = stacked.reshape(levels, HEAD_ROWS, LOW).transpose(1, 0, 2)
    return table.reshape(HEAD_ROWS, levels * LOW)[:HEADS, :entries]


def bit_count(size):
    return size.bit_length() - 1


def exchange_kernel(lat_bits, lon_bits, chunks, factor, grad_ref, table_ref, weight_ref, first_ref,
                    second_ref, new_ref, first_out, second_out, table_out, *scratch):
    bits = lat_bits + lon_bits
    lat, lon = lax.axis_index("lat"), lax.axis_index("lon")
    mine, partner = [], []
    for b in range(bits):
        if b < lat_bits:
            step = 1 << (lat_bits - 1 - b)
            bit = lax.rem(lat // step, 2)
            partner.append({"lat": lat + step * (1 - 2 * bit), "lon": lon})
        else:
            step = 1 << (bits - 1 - b)
            bit = lax.rem(lon // step, 2)
            partner.append({"lat": lat, "lon": lon + step * (1 - 2 * bit)})
        mine.append(bit)
    core, inner = bits - 1, list(range(lat_bits, bits - 1))[::-1]
    ahead, back = list(range(lat_bits))[::-1], list(range(lat_bits))
    orders = [[core] + (ahead if i % 2 == 0 else back) + inner for i in range(len(chunks))]
    held = [scratch[i * bits : (i + 1) * bits] for i in range(len(chunks))]
    table_held = scratch[len(chunks) * bits]
    own_weight, rs_send, rs_recv, ag_send, ag_recv, t_send, t_recv, w_sem = scratch[len(chunks) * bits + 1 :]

    barrier = pltpu.get_barrier_semaphore()
    for b in range(bits):
        pl.semaphore_signal(barrier, inc=1, device_id=partner[b], device_id_type=pl.DeviceIdType.MESH)
    pl.semaphore_wait(barrier, bits)

    def copy(src, dst, send, recv, b):
        return pltpu.make_async_remote_copy(
            src_ref=src, dst_ref=dst, send_sem=send, recv_sem=recv,
            device_id=partner[b], device_id_type=pl.DeviceIdType.MESH)

    def select(dims, b, value):
        return tuple(value if d == b else slice(None) for d in dims)

    def reduce_copy(i, s):
        order, (start, rows) = orders[i], chunks[i]
        b = order[s]
        dims = sorted(order[s:])
        if s == 0:
            src = grad_ref.at[select(dims, b, 1 - mine[b]) + (pl.ds(start, rows),)]
        else:
            src = held[i][s - 1].at[select(dims, b, 1 - mine[b])]
        return copy(src, held[i][s], rs_send.at[i, s], rs_recv.at[i, s], b)

    def reduce_add(i, s):
        order, (start, rows) = orders[i], chunks[i]
        b = order[s]
        dims = sorted(order[s:])
        if s == 0:
            kept = grad_ref[select(dims, b, mine[b]) + (pl.ds(start, rows),)]
        else:
            kept = held[i][s - 1][select(dims, b, mine[b])]
        held[i][s][...] += kept

    def gather_copy(i, s):
        order, (start, rows) = orders[i], chunks[i]
        known = set(order[s + 1 :])
        index = tuple(slice(None) if d in known else mine[d] for d in range(bits))
        region = new_ref.at[index + (pl.ds(start, rows),)]
        return copy(region, region, ag_send.at[i, s], ag_recv.at[i, s], order[s])

    def table_copy(s):
        return copy(table_out if s else table_ref, table_held.at[s], t_send.at[s], t_recv.at[s], orders[0][s])

    fetch = pltpu.make_async_copy(weight_ref.at[tuple(mine)], own_weight, w_sem)
    fetch.start()
    n = len(chunks)
    live = {}
    for i in range(n):
        live[i] = reduce_copy(i, 0)
        live[i].start()
    table_live = table_copy(0)
    table_live.start()
    for s in range(bits):
        for i in range(n):
            live[i].wait()
            reduce_add(i, s)
            if s + 1 < bits:
                live[i] = reduce_copy(i, s + 1)
                live[i].start()
            else:
                if i == 0:
                    fetch.wait()
                rows = pl.ds(*chunks[i])
                grad = held[i][s][...] * factor
                first = 0.9 * first_ref[rows] + 0.1 * grad
                second = 0.95 * second_ref[rows] + 0.05 * grad * grad
                first_out[rows] = first
                second_out[rows] = second
                new_ref[tuple(mine) + (rows,)] = own_weight[rows] - 0.01 * first / (jnp.sqrt(second) + 1e-08)
                live[i] = gather_copy(i, s)
                live[i].start()
        table_live.wait()
        if s == 0:
            table_out[...] = table_ref[...] + table_held[s]
        else:
            table_out[...] += table_held[s]
        if s + 1 < bits:
            table_live = table_copy(s + 1)
            table_live.start()
    table_out[...] *= factor
    for s in reversed(range(bits)):
        for i in range(n):
            live[i].wait()
            if s > 0:
                live[i] = gather_copy(i, s - 1)
                live[i].start()


def chunk_rows(rows, count):
    groups = -(-rows // 8)
    edges = [min(8 * (groups * i // count), rows) for i in range(count)] + [rows]
    return [(a, b - a) for a, b in zip(edges, edges[1:])]


def reduce_update_gather(grads, table, weights, first, second, factor):
    lat_bits, lon_bits = bit_count(lax.axis_size("lat")), bit_count(lax.axis_size("lon"))
    bits = lat_bits + lon_bits
    rows = first.shape[0] // LANES
    chunks = chunk_rows(rows, CHUNKS)
    split_shape = (2,) * bits + (rows, LANES)
    held = [
        pltpu.VMEM((2,) * (bits - 1 - s) + (count, LANES), F32)
        for _, count in chunks
        for s in range(bits)
    ]
    vmem = pl.BlockSpec(memory_space=pltpu.VMEM)
    shard = jax.ShapeDtypeStruct((rows, LANES), F32)
    dma = pltpu.SemaphoreType.DMA
    new, first_new, second_new, table_sum = pl.pallas_call(
        functools.partial(exchange_kernel, lat_bits, lon_bits, chunks, factor),
        in_specs=[vmem, vmem, pl.BlockSpec(memory_space=pl.ANY), vmem, vmem],
        out_specs=[vmem] * 4,
        out_shape=[jax.ShapeDtypeStruct(split_shape, F32), shard, shard,
                   jax.ShapeDtypeStruct(table.shape, F32)],
        scratch_shapes=held + [
            pltpu.VMEM((bits,) + table.shape, F32),
            pltpu.VMEM((rows, LANES), F32),
            dma((len(chunks), bits)), dma((len(chunks), bits)),
            dma((len(chunks), bits)), dma((len(chunks), bits)),
            dma((bits,)), dma((bits,)), dma(()),
        ],
        compiler_params=pltpu.CompilerParams(
            collective_id=0, has_side_effects=True, vmem_limit_bytes=56 * 1024 * 1024),
    )(grads.reshape(split_shape), table, weights.reshape(split_shape),
      first.reshape(rows, LANES), second.reshape(rows, LANES))
    return new.reshape(-1), first_new.reshape(-1), second_new.reshape(-1), table_sum


def shift_ahead(stacked):
    from_east = passed_along(stacked[:, :, :SHIFT], "lon", -1)
    widened = jnp.concatenate([stacked[:, :, SHIFT:], from_east], axis=2)
    from_south = passed_along(widened[:, :SHIFT], "lat", -1)
    return jnp.concatenate([widened[:, SHIFT:], from_south], axis=1)


def shift_back(stacked):
    from_north = passed_along(stacked[:, -SHIFT:], "lat", 1)
    lengthened = jnp.concatenate([from_north, stacked[:, :-SHIFT]], axis=1)
    from_west = passed_along(lengthened[:, :, -SHIFT:], "lon", 1)
    return jnp.concatenate([from_west, lengthened[:, :, :-SHIFT]], axis=2)


def dense(a, b, dims):
    return lax.dot_general(a, b, dims, precision=high, preferred_element_type=F32)


def normalize(values):
    center = values - jnp.mean(values, axis=-1, keepdims=True)
    spread = jnp.mean(center * center, axis=-1, keepdims=True)
    inverse = 1.0 / jnp.sqrt(spread + 1e-05)
    return center * inverse, inverse


def normalize_backward(grad, normed, inverse):
    return inverse * (
        grad
        - jnp.mean(grad, axis=-1, keepdims=True)
        - normed * jnp.mean(grad * normed, axis=-1, keepdims=True)
    )


def per_device(
    block_input, cotangent, weights, first_moment, second_moment, bias_table, bias_index, region_ids
):
    tile_rows, tile_cols, _ = block_input.shape
    lat_count = lax.axis_size("lat")
    lon_count = lax.axis_size("lon")
    tokens = tile_rows * tile_cols
    entries = bias_table.shape[1]
    global_rows = lax.axis_index("lat") * tile_rows + jnp.arange(tile_rows)
    wrapped = global_rows >= tile_rows * lat_count - SHIFT
    labels = region_ids * 2 + wrapped[:, None].astype(jnp.int32)
    labels = windows(labels[:, :, None])[:, :, 0]

    bias = look_up(bias_table, bias_index)
    w_qkv, w_proj, w_up, w_down = unpack(weights)

    moved = shift_ahead(jnp.stack([block_input, cotangent]))
    x = windows(moved[0]).reshape(tokens, D)
    ct = windows(moved[1]).reshape(tokens, D)

    x_normed, x_inverse = normalize(x)
    qkv = dense(x_normed, w_qkv, NN).reshape(-1, TOK, 3 * D)
    context, prob = attention_forward(qkv, bias, labels[:, None, :], labels[:, :, None])
    context = context.reshape(tokens, D)
    mixed = x + dense(context, w_proj, NN)
    m_normed, m_inverse = normalize(mixed)
    hidden, gelu_back = jax.vjp(
        functools.partial(jax.nn.gelu, approximate=True), dense(m_normed, w_up, NN)
    )
    grad_down = dense(hidden, ct, TN)
    (d_up,) = gelu_back(dense(ct, w_down, NT))
    grad_up = dense(m_normed, d_up, TN)
    d_mixed = ct + normalize_backward(dense(d_up, w_up, NT), m_normed, m_inverse)
    grad_proj = dense(context, d_mixed, TN)
    d_context = dense(d_mixed, w_proj, NT).reshape(-1, TOK, D)
    d_qkv, d_bias = attention_backward(qkv, prob, d_context)
    d_qkv = d_qkv.reshape(tokens, 3 * D)
    grad_qkv = dense(x_normed, d_qkv, TN)
    grad_weights = jnp.concatenate(
        [g.reshape(-1) for g in (grad_qkv, grad_proj, grad_up, grad_down)]
    )

    factor = 1.0 / math.sqrt(tokens * lat_count * lon_count)
    dx = d_mixed + normalize_backward(dense(d_qkv, w_qkv, NT), x_normed, x_inverse)
    dx = unwindow(dx.reshape(-1, TOK, D), tile_rows, tile_cols)
    grad_input = shift_back(dx[None])[0]
    table = table_gradient(d_bias, bias_index, entries)
    gathered, first_new, second_new, table = reduce_update_gather(
        grad_weights, table.reshape(-1, LANES), weights, first_moment, second_moment, factor
    )
    table_grad = unstack_table(table.reshape(-1, LOW), entries)
    return (grad_input, gathered, first_new, second_new, table_grad)


def solution(mesh):
    placed = (
        P("lat", "lon", None),
        P("lat", "lon", None),
        P(),
        P(("lat", "lon")),
        P(("lat", "lon")),
        P(),
        P(),
        P("lat", "lon"),
    )
    return jax.shard_map(
        per_device,
        mesh=mesh,
        in_specs=placed,
        out_specs=(P("lat", "lon", None), P(), P(("lat", "lon")), P(("lat", "lon")), P()),
        check_vma=False,
    )
```

```python
import functools
import math

import jax
import jax.numpy as jnp
from jax import lax
from jax.experimental import pallas as pl
from jax.experimental.pallas import tpu as pltpu
from jax.sharding import PartitionSpec as P

D = 384
HEADS = 12
FF = 1536
WIN = 12
HEAD_DIM = 32
SHIFT = 6
TOK = WIN * WIN
HEAD_ROWS = 16
LANES = 128
PACK = LANES // HEAD_DIM
EDGE = 8
FF_BLOCK = 512
CHUNKS = 4
SCALE = 1.0 / math.sqrt(HEAD_DIM)

F32 = jnp.float32
BF16 = jnp.bfloat16
NN = (((1,), (0,)), ((), ()))
NT = (((1,), (1,)), ((), ()))
VMEM_LIMIT = 63 * 1024 * 1024

def split(value):
    upper = value.astype(BF16)
    return upper, (value - upper.astype(F32)).astype(BF16)


def mul(a, b, dims):
    return lax.dot_general(a, b, dims, preferred_element_type=F32)


def dot_nn(a, b):
    return mul(jnp.concatenate([a[0], a[0], a[1]], 1), jnp.concatenate([b[0], b[1], b[0]], 0), NN)


def dot_nt(a, b):
    return mul(jnp.concatenate([a[0], a[0], a[1]], 1), jnp.concatenate([b[0], b[1], b[0]], 1), NT)


def dot_rows(a, b):
    rows = a[0].shape[0]
    both = mul(jnp.concatenate([a[0], a[1]], 0), b[0], NN)
    return both[:rows] + both[rows:] + mul(a[0], b[1], NN)


def dot_cols(a, b):
    cols = b[0].shape[1]
    both = mul(a[0], jnp.concatenate([b[0], b[1]], 1), NN)
    return both[:, :cols] + both[:, cols:] + mul(a[1], b[0], NN)


def normalize(values):
    center = values - jnp.mean(values, axis=-1, keepdims=True)
    spread = jnp.mean(center * center, axis=-1, keepdims=True)
    inverse = 1.0 / jnp.sqrt(spread + 1e-05)
    return center * inverse, inverse


def normalize_backward(grad, normed, inverse):
    return inverse * (
        grad
        - jnp.mean(grad, axis=-1, keepdims=True)
        - normed * jnp.mean(grad * normed, axis=-1, keepdims=True)
    )


def gelu_and_slope(u):
    c = math.sqrt(2.0 / math.pi)
    square = u * u
    t = jnp.tanh(c * u * (1.0 + 0.044715 * square))
    half = 0.5 * (1.0 + t)
    slope = half + 0.5 * u * (1.0 - t * t) * (c * (1.0 + 3.0 * 0.044715 * square))
    return u * half, slope


def window_pieces(height, breadth):
    at = 0
    for r in range(height // WIN):
        for c in range(breadth // WIN):
            for i in range(WIN):
                yield at, SHIFT + r * WIN + i, SHIFT + c * WIN
                at += WIN


def halo_kernel(x_ref, ct_ref, xw_ref, ctw_ref, wide, send, recv, local):
    height, breadth, _ = x_ref.shape
    barrier = pltpu.get_barrier_semaphore()
    for where in neighbours(1):
        pl.semaphore_signal(barrier, inc=1, device_id=where, device_id_type=pl.DeviceIdType.MESH)
    pl.semaphore_wait(barrier, 3)
    copies = []
    for n, ref in enumerate((x_ref, ct_ref)):
        parts = (
            (ref.at[:, pl.ds(0, EDGE)], wide.at[n, pl.ds(0, height), pl.ds(breadth, EDGE)]),
            (ref.at[pl.ds(0, SHIFT)], wide.at[n, pl.ds(height, SHIFT), pl.ds(0, breadth)]),
            (ref.at[pl.ds(0, SHIFT), pl.ds(0, EDGE)],
             wide.at[n, pl.ds(height, SHIFT), pl.ds(breadth, EDGE)]),
        )
        for k, ((src, dst), where) in enumerate(zip(parts, neighbours(-1))):
            copies.append(pltpu.make_async_remote_copy(
                src_ref=src, dst_ref=dst, send_sem=send.at[n, k], recv_sem=recv.at[n, k],
                device_id=where, device_id_type=pl.DeviceIdType.MESH))
        copies.append(pltpu.make_async_copy(
            ref, wide.at[n, pl.ds(0, height), pl.ds(0, breadth)], local.at[n]))
    for copy in copies:
        copy.start()
    for copy in copies:
        copy.wait()
    for n, out in enumerate((xw_ref, ctw_ref)):
        for at, row, col in window_pieces(height, breadth):
            out[at : at + WIN] = wide[n, row, col : col + WIN]


def gather_windows(block_input, cotangent):
    height, breadth, _ = block_input.shape
    dma = pltpu.SemaphoreType.DMA
    return pl.pallas_call(
        halo_kernel,
        in_specs=[pl.BlockSpec(memory_space=pl.ANY)] * 2,
        out_specs=[pl.BlockSpec(memory_space=pltpu.VMEM)] * 2,
        out_shape=[jax.ShapeDtypeStruct((height * breadth, D), F32)] * 2,
        scratch_shapes=[
            pltpu.VMEM((2, height + SHIFT, breadth + EDGE, D), F32),
            dma((2, 3)), dma((2, 3)), dma((2,)),
        ],
        compiler_params=pltpu.CompilerParams(collective_id=1, has_side_effects=True),
    )(block_input, cotangent)


def block_kernel(x_ref, ct_ref, w_ref, table_ref, index_ref, region_ref, grad_ref, edge_ref,
                 table_out, wq, wp, wu, wd, table, index, bias, dbias, prob, xn_s, mn_s, ct_s,
                 qkv_s, q_s, ctx_s, d_s, turned, acc, labels, dqkv_s, spread):
    height, breadth = region_ref.shape
    across = breadth // WIN
    tokens = x_ref.shape[0]
    count = tokens // TOK
    heads, entries = table_ref.shape
    levels = table.shape[1] // LANES
    row_of = [0, D * 3 * D // LANES, (D * 3 * D + D * D) // LANES, (D * 3 * D + D * D + D * FF) // LANES]

    def put(ref, rows, value):
        upper, lower = split(value)
        ref[0, rows], ref[1, rows] = upper, lower

    def pair(ref, *at):
        return ref[(0,) + at], ref[(1,) + at]

    def full(ref):
        return ref[0].astype(F32) + ref[1].astype(F32)

    for dst, start in zip((wq, wp, wu, wd), row_of):
        _, rows, width = dst.shape
        blocks = width // LANES
        for j in range(blocks):
            upper, lower = split(w_ref[pl.ds(start + j, rows, stride=blocks), :])
            dst[0, :, j * LANES : (j + 1) * LANES] = upper
            dst[1, :, j * LANES : (j + 1) * LANES] = lower

    table[...] = jnp.zeros_like(table)
    table[:heads, :entries] = table_ref[...]
    index[...] = jnp.zeros_like(index)
    index[:, :TOK] = index_ref[...]

    def look_up(block, carry):
        rows = pl.ds(pl.multiple_of(block * 8, 8), 8)
        for side in range(2):
            at = index[rows, side * LANES : (side + 1) * LANES]
            low, level_of = at & (LANES - 1), at >> 7
            width = min(LANES, TOK - side * LANES)
            for h in range(heads):
                total = jnp.zeros((8, LANES), F32)
                for level in range(levels):
                    source = jnp.broadcast_to(
                        table[h : h + 1, level * LANES : (level + 1) * LANES], (8, LANES))
                    found = jnp.take_along_axis(source, low, axis=1, mode="promise_in_bounds")
                    total = jnp.where(level_of == level, found, total)
                bias[h, rows, side * LANES : side * LANES + width] = total[:, :width]
        return carry

    lax.fori_loop(0, TOK // 8, look_up, 0)

    lat = lax.axis_index("lat")
    grid_row = lat * height + lax.broadcasted_iota(jnp.int32, (height, breadth), 0)
    wrapped = (grid_row >= height * lax.axis_size("lat") - SHIFT).astype(jnp.int32)
    labels[...] = (region_ref[...] * 2 + wrapped).astype(F32)

    x = x_ref[...]
    x_normed, x_inverse = normalize(x)
    put(xn_s, slice(None), x_normed)
    spread[0] = jnp.broadcast_to(x_inverse, (tokens, LANES))
    qkv = dot_nn(pair(xn_s), pair(wq))
    q = qkv[:, :D] * SCALE
    q_s[...] = q
    for j, part in enumerate((q, qkv[:, D : 2 * D], qkv[:, 2 * D :])):
        upper, lower = split(part)
        qkv_s[0, :, j * D : (j + 1) * D] = upper
        qkv_s[1, :, j * D : (j + 1) * D] = lower
    put(ct_s, slice(None), ct_ref[...])

    lane_head = lax.broadcasted_iota(jnp.int32, (TOK, LANES), 1) >> 5

    def only(head, values):
        keep = lane_head == head
        return tuple(jnp.where(keep, v, jnp.zeros_like(v)) for v in values)

    def tile(which, t, rows):
        cols = slice(which * D + t * LANES, which * D + (t + 1) * LANES)
        return qkv_s[0, rows, cols], qkv_s[1, rows, cols]

    def forward(w, carry):
        rows = pl.ds(pl.multiple_of(w * TOK, TOK), TOK)
        first_row, first_col = (w // across) * WIN, (w % across) * WIN
        position = lax.broadcasted_iota(jnp.int32, (TOK, height), 0)
        quotient = (position * 171) >> 11
        hot = (lax.broadcasted_iota(jnp.int32, (TOK, height), 1) == quotient + first_row).astype(F32)
        picked = mul(hot.astype(BF16), labels[...].astype(BF16), NN)
        position = lax.broadcasted_iota(jnp.int32, (TOK, breadth), 0)
        rest = position - WIN * ((position * 171) >> 11)
        chosen = lax.broadcasted_iota(jnp.int32, (TOK, breadth), 1) == rest + first_col
        label = jnp.sum(jnp.where(chosen, picked, 0.0), axis=1, keepdims=True)
        across_label = jnp.transpose(jnp.broadcast_to(label, (TOK, LANES)))[:1]
        allowed = label == across_label
        for t in range(D // LANES):
            q, k, v = (tile(j, t, rows) for j in range(3))
            total = jnp.zeros((TOK, LANES), F32)
            for head in range(PACK):
                h = t * PACK + head
                scores = dot_nt(only(head, q), k) + bias[h]
                masked = jnp.where(allowed, scores, -jnp.inf)
                raised = jnp.exp(masked - jnp.max(masked, axis=-1, keepdims=True))
                p = split(raised * (1.0 / jnp.sum(raised, axis=-1, keepdims=True)))
                prob[0, w * heads + h], prob[1, w * heads + h] = p
                total += dot_cols(p, only(head, v))
            ctx_s[rows, t * LANES : (t + 1) * LANES] = total
        return carry

    lax.fori_loop(0, count, forward, 0)

    mixed = x_ref[...] + dot_nn(split(ctx_s[...]), pair(wp))
    m_normed, m_inverse = normalize(mixed)
    put(mn_s, slice(None), m_normed)
    spread[1] = jnp.broadcast_to(m_inverse, (tokens, LANES))
    for n, value in enumerate((m_normed, ct_ref[...])):
        turned[n, 0], turned[n, 1] = split(jnp.transpose(value))
    acc[...] = jnp.zeros_like(acc)

    def feed(f, carry):
        cols = pl.ds(pl.multiple_of(f * FF_BLOCK, FF_BLOCK), FF_BLOCK)
        w_up = pair(wu, slice(None), cols)
        hidden, slope = gelu_and_slope(dot_nn(pair(mn_s), w_up))
        d_up = split(dot_nt(pair(ct_s), pair(wd, cols)) * slope)
        hidden = split(hidden)
        blocks = FF // LANES
        grad = dot_rows((turned[0, 0], turned[0, 1]), d_up)
        for j in range(FF_BLOCK // LANES):
            start = row_of[2] + f * (FF_BLOCK // LANES) + j
            grad_ref[pl.ds(start, D, stride=blocks), :] = grad[:, j * LANES : (j + 1) * LANES]
        grad = jnp.transpose(dot_rows((turned[1, 0], turned[1, 1]), hidden))
        blocks = D // LANES
        for j in range(blocks):
            start = row_of[3] + f * (FF_BLOCK * blocks) + j
            grad_ref[pl.ds(start, FF_BLOCK, stride=blocks), :] = grad[:, j * LANES : (j + 1) * LANES]
        acc[...] += dot_nt(d_up, w_up)
        return carry

    lax.fori_loop(0, FF // FF_BLOCK, feed, 0)

    d_mixed = ct_ref[...] + normalize_backward(acc[...], full(mn_s), spread[1][:, :1])
    acc[...] = d_mixed
    d_pair = split(d_mixed)
    turned[0, 0], turned[0, 1] = split(jnp.transpose(ctx_s[...]))
    grad = dot_rows((turned[0, 0], turned[0, 1]), d_pair)
    blocks = D // LANES
    for j in range(blocks):
        grad_ref[pl.ds(row_of[1] + j, D, stride=blocks), :] = grad[:, j * LANES : (j + 1) * LANES]
    d_s[...] = dot_nt(d_pair, pair(wp))
    dbias[...] = jnp.zeros_like(dbias)

    def backward(w, carry):
        rows = pl.ds(pl.multiple_of(w * TOK, TOK), TOK)
        for t in range(D // LANES):
            cols = slice(t * LANES, (t + 1) * LANES)
            k, v = tile(1, t, rows), tile(2, t, rows)
            grad = d_s[rows, cols]
            weighed = grad * ctx_s[rows, cols]
            g = split(grad)
            g_turned = split(jnp.transpose(grad))
            q_turned = split(jnp.transpose(q_s[rows, cols]))
            dq = jnp.zeros((TOK, LANES), F32)
            dk, dv = [], []
            for head in range(PACK):
                h = t * PACK + head
                part = slice(head * HEAD_DIM, (head + 1) * HEAD_DIM)
                upper, lower = prob[0, w * heads + h], prob[1, w * heads + h]
                dprob = dot_nt(only(head, g), v)
                delta = jnp.sum(jnp.where(lane_head == head, weighed, 0.0), axis=-1, keepdims=True)
                dscore = (upper.astype(F32) + lower.astype(F32)) * (dprob - delta)
                dbias[h] += dscore
                ds = split(dscore)
                dq += dot_cols(ds, only(head, k))
                dk.append(dot_rows((q_turned[0][part], q_turned[1][part]), ds))
                dv.append(dot_rows((g_turned[0][part], g_turned[1][part]), (upper, lower)))
            for j, value in enumerate((dq * SCALE, jnp.transpose(jnp.concatenate(dk, 0)),
                                       jnp.transpose(jnp.concatenate(dv, 0)))):
                at = slice(j * D + t * LANES, j * D + (t + 1) * LANES)
                upper, lower = split(value)
                dqkv_s[0, rows, at], dqkv_s[1, rows, at] = upper, lower
        return carry

    lax.fori_loop(0, count, backward, 0)

    x_normed = full(xn_s)
    turned[1, 0], turned[1, 1] = split(jnp.transpose(x_normed))
    grad = dot_rows((turned[1, 0], turned[1, 1]), pair(dqkv_s))
    blocks = 3 * D // LANES
    for j in range(blocks):
        grad_ref[pl.ds(row_of[0] + j, D, stride=blocks), :] = grad[:, j * LANES : (j + 1) * LANES]
    d_normed = dot_nt(pair(dqkv_s), pair(wq))
    q_s[...] = acc[...] + normalize_backward(d_normed, x_normed, spread[0][:, :1])
    edge_ref[...] = jnp.zeros_like(edge_ref)
    for at, row, col in window_pieces(height, breadth):
        edge_ref[row, col : col + WIN] = q_s[at : at + WIN]

    table_acc = jnp.zeros((levels * 2 * HEAD_ROWS, LANES), F32)

    def collect(block, total):
        rows = pl.ds(pl.multiple_of(block * 8, 8), 8)
        at_rows = index_ref[rows, :]
        grads = dbias[:, rows, :]
        for r in range(8):
            at = at_rows[r : r + 1]
            low, level_of = at & (LANES - 1), at >> 7
            grad = jnp.concatenate([grads[:, r, :], jnp.zeros((HEAD_ROWS - heads, TOK), F32)], 0)
            stacked = jnp.concatenate(
                [jnp.where(level_of == level, grad, 0.0) for level in range(levels)], 0)
            hot = (lax.broadcasted_iota(jnp.int32, (LANES, TOK), 0) == low).astype(F32).astype(BF16)
            total = total + mul(jnp.concatenate(split(stacked), 0), hot, NT)
        return total

    total = lax.fori_loop(0, TOK // 8, collect, table_acc)
    table_out[...] = total[: levels * HEAD_ROWS] + total[levels * HEAD_ROWS :]


def block_gradients(x, ct, weights, bias_table, bias_index, region_ids):
    tokens = x.shape[0]
    height, breadth = region_ids.shape
    heads, entries = bias_table.shape
    levels = -(-entries // LANES)
    count = tokens // TOK
    vmem = pl.BlockSpec(memory_space=pltpu.VMEM)
    return pl.pallas_call(
        block_kernel,
        in_specs=[vmem] * 6,
        out_specs=[vmem] * 3,
        out_shape=[
            jax.ShapeDtypeStruct((weights.shape[0] // LANES, LANES), F32),
            jax.ShapeDtypeStruct((height + SHIFT, breadth + EDGE, D), F32),
            jax.ShapeDtypeStruct((levels * HEAD_ROWS, LANES), F32),
        ],
        scratch_shapes=[
            pltpu.VMEM((2, D, 3 * D), BF16),
            pltpu.VMEM((2, D, D), BF16),
            pltpu.VMEM((2, D, FF), BF16),
            pltpu.VMEM((2, FF, D), BF16),
            pltpu.VMEM((HEAD_ROWS, levels * LANES), F32),
            pltpu.VMEM((TOK, 2 * LANES), jnp.int32),
            pltpu.VMEM((heads, TOK, TOK), F32),
            pltpu.VMEM((heads, TOK, TOK), F32),
            pltpu.VMEM((2, count * heads, TOK, TOK), BF16),
            pltpu.VMEM((2, tokens, D), BF16),
            pltpu.VMEM((2, tokens, D), BF16),
            pltpu.VMEM((2, tokens, D), BF16),
            pltpu.VMEM((2, tokens, 3 * D), BF16),
            pltpu.VMEM((tokens, D), F32),
            pltpu.VMEM((tokens, D), F32),
            pltpu.VMEM((tokens, D), F32),
            pltpu.VMEM((2, 2, D, tokens), BF16),
            pltpu.VMEM((tokens, D), F32),
            pltpu.VMEM((height, breadth), F32),
            pltpu.VMEM((2, tokens, 3 * D), BF16),
            pltpu.VMEM((2, tokens, LANES), F32),
        ],
        compiler_params=pltpu.CompilerParams(vmem_limit_bytes=VMEM_LIMIT),
    )(x, ct, weights.reshape(-1, LANES), bias_table, bias_index, region_ids)


def bit_count(size):
    return size.bit_length() - 1


def neighbours(by):
    lat_size, lon_size = lax.axis_size("lat"), lax.axis_size("lon")
    lat = lax.rem(lax.axis_index("lat") + by + lat_size, lat_size)
    lon = lax.rem(lax.axis_index("lon") + by + lon_size, lon_size)
    return ({"lon": lon}, {"lat": lat}, {"lat": lat, "lon": lon})


def exchange_kernel(lat_bits, lon_bits, chunks, factor, grad_ref, table_ref, edge_ref, weight_ref,
                    first_ref, second_ref, new_ref, first_out, second_out, table_final, dx_out, *scratch):
    bits = lat_bits + lon_bits
    lat, lon = lax.axis_index("lat"), lax.axis_index("lon")
    mine, partner = [], []
    for b in range(bits):
        if b < lat_bits:
            step = 1 << (lat_bits - 1 - b)
            bit = lax.rem(lat // step, 2)
            partner.append({"lat": lat + step * (1 - 2 * bit), "lon": lon})
        else:
            step = 1 << (bits - 1 - b)
            bit = lax.rem(lon // step, 2)
            partner.append({"lat": lat, "lon": lon + step * (1 - 2 * bit)})
        mine.append(bit)
    core, inner = bits - 1, list(range(lat_bits, bits - 1))[::-1]
    ahead, back = list(range(lat_bits))[::-1], list(range(lat_bits))
    orders = [[core] + (ahead if i % 2 == 0 else back) + inner for i in range(len(chunks))]
    held = [scratch[i * bits : (i + 1) * bits] for i in range(len(chunks))]
    table_held, table_out = scratch[len(chunks) * bits : len(chunks) * bits + 2]
    west_in, north_in, corner_in, own_weight, rs_send, rs_recv, ag_send, ag_recv, t_send, t_recv, e_send, e_recv, w_sem = scratch[
        len(chunks) * bits + 2 :
    ]

    barrier = pltpu.get_barrier_semaphore()
    for b in range(bits):
        pl.semaphore_signal(barrier, inc=1, device_id=partner[b], device_id_type=pl.DeviceIdType.MESH)
    for where in neighbours(-1):
        pl.semaphore_signal(barrier, inc=1, device_id=where, device_id_type=pl.DeviceIdType.MESH)
    pl.semaphore_wait(barrier, bits + 3)

    height, breadth, _ = dx_out.shape
    edges = [
        pltpu.make_async_remote_copy(
            src_ref=src, dst_ref=dst, send_sem=e_send.at[n], recv_sem=e_recv.at[n],
            device_id=where, device_id_type=pl.DeviceIdType.MESH)
        for n, (src, dst, where) in enumerate(zip(
            (edge_ref.at[pl.ds(SHIFT, height - SHIFT), pl.ds(breadth, EDGE)],
             edge_ref.at[pl.ds(height, SHIFT), pl.ds(0, breadth)],
             edge_ref.at[pl.ds(height, SHIFT), pl.ds(breadth, EDGE)]),
            (west_in, north_in, corner_in), neighbours(1)))
    ]

    def copy(src, dst, send, recv, b):
        return pltpu.make_async_remote_copy(
            src_ref=src, dst_ref=dst, send_sem=send, recv_sem=recv,
            device_id=partner[b], device_id_type=pl.DeviceIdType.MESH)

    def select(dims, b, value):
        return tuple(value if d == b else slice(None) for d in dims)

    def reduce_copy(i, s):
        order, (start, rows) = orders[i], chunks[i]
        b = order[s]
        dims = sorted(order[s:])
        if s == 0:
            src = grad_ref.at[select(dims, b, 1 - mine[b]) + (pl.ds(start, rows),)]
        else:
            src = held[i][s - 1].at[select(dims, b, 1 - mine[b])]
        return copy(src, held[i][s], rs_send.at[i, s], rs_recv.at[i, s], b)

    def reduce_add(i, s):
        order, (start, rows) = orders[i], chunks[i]
        b = order[s]
        dims = sorted(order[s:])
        if s == 0:
            kept = grad_ref[select(dims, b, mine[b]) + (pl.ds(start, rows),)]
        else:
            kept = held[i][s - 1][select(dims, b, mine[b])]
        held[i][s][...] += kept

    def gather_copy(i, s):
        order, (start, rows) = orders[i], chunks[i]
        known = set(order[s + 1 :])
        index = tuple(slice(None) if d in known else mine[d] for d in range(bits))
        region = new_ref.at[index + (pl.ds(start, rows),)]
        return copy(region, region, ag_send.at[i, s], ag_recv.at[i, s], order[s])

    def table_copy(s):
        return copy(table_out if s else table_ref, table_held.at[s], t_send.at[s], t_recv.at[s], orders[0][s])

    fetch = pltpu.make_async_copy(weight_ref.at[tuple(mine)], own_weight, w_sem)
    fetch.start()
    n = len(chunks)
    live = {}
    for i in range(n):
        live[i] = reduce_copy(i, 0)
        live[i].start()
    table_live = table_copy(0)
    table_live.start()
    for edge in edges:
        edge.start()
    for s in range(bits):
        for i in range(n):
            live[i].wait()
            reduce_add(i, s)
            if s + 1 < bits:
                live[i] = reduce_copy(i, s + 1)
                live[i].start()
            else:
                if i == 0:
                    fetch.wait()
                rows = pl.ds(*chunks[i])
                grad = held[i][s][...] * factor
                first = 0.9 * first_ref[rows] + 0.1 * grad
                second = 0.95 * second_ref[rows] + 0.05 * grad * grad
                first_out[rows] = first
                second_out[rows] = second
                new_ref[tuple(mine) + (rows,)] = own_weight[rows] - 0.01 * first / (jnp.sqrt(second) + 1e-08)
                live[i] = gather_copy(i, s)
                live[i].start()
        table_live.wait()
        if s == 0:
            table_out[...] = table_ref[...] + table_held[s]
        else:
            table_out[...] += table_held[s]
        if s + 1 < bits:
            table_live = table_copy(s + 1)
            table_live.start()
    heads, entries = table_final.shape
    for level in range(-(-entries // LANES)):
        width = min(LANES, entries - level * LANES)
        table_final[:, pl.ds(level * LANES, width)] = (
            table_out[pl.ds(level * HEAD_ROWS, heads), pl.ds(0, width)] * factor
        )
    for edge in edges:
        edge.wait()
    dx_out[SHIFT:, EDGE:] = edge_ref[SHIFT:height, EDGE:breadth]
    dx_out[:SHIFT, EDGE:] = north_in[:, EDGE:]
    column = lax.broadcasted_iota(jnp.int32, (1, EDGE, D), 1)
    dx_out[SHIFT:, :EDGE] = jnp.where(column < SHIFT, west_in[...], edge_ref[SHIFT:height, :EDGE])
    dx_out[:SHIFT, :EDGE] = jnp.where(column < SHIFT, corner_in[...], north_in[:, :EDGE])
    for s in reversed(range(bits)):
        for i in range(n):
            live[i].wait()
            if s > 0:
                live[i] = gather_copy(i, s - 1)
                live[i].start()


def chunk_rows(rows, count):
    groups = -(-rows // 8)
    edges = [min(8 * (groups * i // count), rows) for i in range(count)] + [rows]
    return [(a, b - a) for a, b in zip(edges, edges[1:])]


def reduce_update_gather(grads, table, edge, weights, first, second, table_shape, tile_shape, factor):
    lat_bits, lon_bits = bit_count(lax.axis_size("lat")), bit_count(lax.axis_size("lon"))
    bits = lat_bits + lon_bits
    rows = first.shape[0] // LANES
    chunks = chunk_rows(rows, CHUNKS)
    split_shape = (2,) * bits + (rows, LANES)
    height, breadth, _ = tile_shape
    held = [
        pltpu.VMEM((2,) * (bits - 1 - s) + (count, LANES), F32)
        for _, count in chunks
        for s in range(bits)
    ]
    vmem = pl.BlockSpec(memory_space=pltpu.VMEM)
    shard = jax.ShapeDtypeStruct((rows, LANES), F32)
    dma = pltpu.SemaphoreType.DMA
    new, first_new, second_new, table_sum, dx = pl.pallas_call(
        functools.partial(exchange_kernel, lat_bits, lon_bits, chunks, factor),
        in_specs=[vmem, vmem, vmem, pl.BlockSpec(memory_space=pl.ANY), vmem, vmem],
        out_specs=[vmem] * 5,
        out_shape=[jax.ShapeDtypeStruct(split_shape, F32), shard, shard,
                   jax.ShapeDtypeStruct(table_shape, F32),
                   jax.ShapeDtypeStruct(tile_shape, F32)],
        scratch_shapes=held + [
            pltpu.VMEM((bits,) + table.shape, F32),
            pltpu.VMEM(table.shape, F32),
            pltpu.VMEM((height - SHIFT, EDGE, D), F32),
            pltpu.VMEM((SHIFT, breadth, D), F32),
            pltpu.VMEM((SHIFT, EDGE, D), F32),
            pltpu.VMEM((rows, LANES), F32),
            dma((len(chunks), bits)), dma((len(chunks), bits)),
            dma((len(chunks), bits)), dma((len(chunks), bits)),
            dma((bits,)), dma((bits,)), dma((3,)), dma((3,)), dma(()),
        ],
        compiler_params=pltpu.CompilerParams(
            collective_id=0, has_side_effects=True, vmem_limit_bytes=56 * 1024 * 1024),
    )(grads.reshape(split_shape), table, edge, weights.reshape(split_shape),
      first.reshape(rows, LANES), second.reshape(rows, LANES))
    return new.reshape(-1), first_new.reshape(-1), second_new.reshape(-1), table_sum, dx


def per_device(
    block_input, cotangent, weights, first_moment, second_moment, bias_table, bias_index, region_ids
):
    tile_rows, tile_cols, _ = block_input.shape
    devices = lax.axis_size("lat") * lax.axis_size("lon")
    factor = 1.0 / math.sqrt(tile_rows * tile_cols * devices)
    x, ct = gather_windows(block_input, cotangent)
    grads, edge, table = block_gradients(x, ct, weights, bias_table, bias_index, region_ids)
    gathered, first_new, second_new, table_grad, grad_input = reduce_update_gather(
        grads, table, edge, weights, first_moment, second_moment, bias_table.shape,
        block_input.shape, factor,
    )
    return (grad_input, gathered, first_new, second_new, table_grad)


def solution(mesh):
    placed = (
        P("lat", "lon", None),
        P("lat", "lon", None),
        P(),
        P(("lat", "lon")),
        P(("lat", "lon")),
        P(),
        P(),
        P("lat", "lon"),
    )
    return jax.shard_map(
        per_device,
        mesh=mesh,
        in_specs=placed,
        out_specs=(P("lat", "lon", None), P(), P(("lat", "lon")), P(("lat", "lon")), P()),
        check_vma=False,
    )
```

```python
import functools
import math

import jax
import jax.numpy as jnp
from jax import lax
from jax.experimental import pallas as pl
from jax.experimental.pallas import tpu as pltpu
from jax.sharding import PartitionSpec as P

D = 384
HEADS = 12
FF = 1536
WIN = 12
HEAD_DIM = 32
SHIFT = 6
TOK = WIN * WIN
HEAD_ROWS = 16
LANES = 128
PACK = LANES // HEAD_DIM
EDGE = 8
FF_BLOCK = 512
CHUNKS = 7
SCALE = 1.0 / math.sqrt(HEAD_DIM)

F32 = jnp.float32
BF16 = jnp.bfloat16
NN = (((1,), (0,)), ((), ()))
NT = (((1,), (1,)), ((), ()))
VMEM_LIMIT = 63 * 1024 * 1024

def neighbours(by):
    lat_size, lon_size = lax.axis_size("lat"), lax.axis_size("lon")
    lat = lax.rem(lax.axis_index("lat") + by + lat_size, lat_size)
    lon = lax.rem(lax.axis_index("lon") + by + lon_size, lon_size)
    return ({"lon": lon}, {"lat": lat}, {"lat": lat, "lon": lon})


def split(value):
    upper = value.astype(BF16)
    return upper, (value - upper.astype(F32)).astype(BF16)


def mul(a, b, dims):
    return lax.dot_general(a, b, dims, preferred_element_type=F32)


def dot_nn(a, b):
    return mul(jnp.concatenate([a[0], a[0], a[1]], 1), jnp.concatenate([b[0], b[1], b[0]], 0), NN)


def dot_nt(a, b):
    return mul(jnp.concatenate([a[0], a[0], a[1]], 1), jnp.concatenate([b[0], b[1], b[0]], 1), NT)


def dot_rows(a, b):
    rows = a[0].shape[0]
    both = mul(jnp.concatenate([a[0], a[1]], 0), b[0], NN)
    return both[:rows] + both[rows:] + mul(a[0], b[1], NN)


def dot_cols(a, b):
    cols = b[0].shape[1]
    both = mul(a[0], jnp.concatenate([b[0], b[1]], 1), NN)
    return both[:, :cols] + both[:, cols:] + mul(a[1], b[0], NN)


def normalize(values):
    center = values - jnp.mean(values, axis=-1, keepdims=True)
    spread = jnp.mean(center * center, axis=-1, keepdims=True)
    inverse = 1.0 / jnp.sqrt(spread + 1e-05)
    return center * inverse, inverse


def normalize_backward(grad, normed, inverse):
    return inverse * (
        grad
        - jnp.mean(grad, axis=-1, keepdims=True)
        - normed * jnp.mean(grad * normed, axis=-1, keepdims=True)
    )


def gelu_and_slope(u):
    c = math.sqrt(2.0 / math.pi)
    square = u * u
    t = jnp.tanh(c * u * (1.0 + 0.044715 * square))
    half = 0.5 * (1.0 + t)
    slope = half + 0.5 * u * (1.0 - t * t) * (c * (1.0 + 3.0 * 0.044715 * square))
    return u * half, slope


def window_pieces(height, breadth):
    at = 0
    for r in range(height // WIN):
        for c in range(breadth // WIN):
            for i in range(WIN):
                yield at, SHIFT + r * WIN + i, SHIFT + c * WIN
                at += WIN


def greet(places):
    barrier = pltpu.get_barrier_semaphore()
    for where in places:
        pl.semaphore_signal(barrier, inc=1, device_id=where, device_id_type=pl.DeviceIdType.MESH)
    pl.semaphore_wait(barrier, len(places))


def halo_copies(n, ref, wide, send, recv, local):
    height, breadth, _ = ref.shape
    parts = (
        (ref.at[:, pl.ds(0, EDGE)], wide.at[n, pl.ds(0, height), pl.ds(breadth, EDGE)]),
        (ref.at[pl.ds(0, SHIFT)], wide.at[n, pl.ds(height, SHIFT), pl.ds(0, breadth)]),
        (ref.at[pl.ds(0, SHIFT), pl.ds(0, EDGE)],
         wide.at[n, pl.ds(height, SHIFT), pl.ds(breadth, EDGE)]),
    )
    copies = [
        pltpu.make_async_remote_copy(
            src_ref=src, dst_ref=dst, send_sem=send.at[n, k], recv_sem=recv.at[n, k],
            device_id=where, device_id_type=pl.DeviceIdType.MESH)
        for k, ((src, dst), where) in enumerate(zip(parts, neighbours(-1)))
    ]
    copies.append(pltpu.make_async_copy(
        ref, wide.at[n, pl.ds(0, height), pl.ds(0, breadth)], local.at[n]))
    for copy in copies:
        copy.start()
    return copies


def assemble(n, copies, shape, wide, out):
    for copy in copies:
        copy.wait()
    for at, row, col in window_pieces(shape[0], shape[1]):
        out[at : at + WIN] = wide[n, row, col : col + WIN]


def halo_kernel(x_ref, ct_ref, xw_ref, ctw_ref, wide, send, recv, local):
    greet(neighbours(1))
    copies = [halo_copies(n, ref, wide, send, recv, local) for n, ref in enumerate((x_ref, ct_ref))]
    for n, out in enumerate((xw_ref, ctw_ref)):
        assemble(n, copies[n], x_ref.shape, wide, out)


def gather_windows(block_input, cotangent):
    height, breadth, _ = block_input.shape
    dma = pltpu.SemaphoreType.DMA
    return pl.pallas_call(
        halo_kernel,
        in_specs=[pl.BlockSpec(memory_space=pl.ANY)] * 2,
        out_specs=[pl.BlockSpec(memory_space=pltpu.VMEM)] * 2,
        out_shape=[jax.ShapeDtypeStruct((height * breadth, D), F32)] * 2,
        scratch_shapes=[
            pltpu.VMEM((2, height + SHIFT, breadth + EDGE, D), F32),
            dma((2, 3)), dma((2, 3)), dma((2,)),
        ],
        compiler_params=pltpu.CompilerParams(collective_id=1, has_side_effects=True),
    )(block_input, cotangent)


def block_steps(x_ref, ct_ref, w_ref, table_ref, index_ref, region_ref, grad_ref, edge_ref,
                table_out, d_s, wq, wp, wu, wd, table, index, bias, prob, xn_s, mn_s, ct_s,
                qkv_s, q_s, ctx_s, turned, acc, labels, spread):
    dbias, dqkv_s = bias, qkv_s
    height, breadth = region_ref.shape
    across = breadth // WIN
    tokens = x_ref.shape[0]
    count = tokens // TOK
    heads, entries = table_ref.shape
    levels = table.shape[1] // LANES
    row_of = [0, D * 3 * D // LANES, (D * 3 * D + D * D) // LANES, (D * 3 * D + D * D + D * FF) // LANES]

    def put(ref, rows, value):
        upper, lower = split(value)
        ref[0, rows], ref[1, rows] = upper, lower

    def pair(ref, *at):
        return ref[(0,) + at], ref[(1,) + at]

    def full(ref):
        return ref[0].astype(F32) + ref[1].astype(F32)

    yield
    for dst, start in zip((wq, wp, wu, wd), row_of):
        _, rows, width = dst.shape
        blocks = width // LANES
        for j in range(blocks):
            upper, lower = split(w_ref[pl.ds(start + j, rows, stride=blocks), :])
            dst[0, :, j * LANES : (j + 1) * LANES] = upper
            dst[1, :, j * LANES : (j + 1) * LANES] = lower

    table[...] = jnp.zeros_like(table)
    table[:heads, :entries] = table_ref[...]
    index[...] = jnp.zeros_like(index)
    index[:, :TOK] = index_ref[...]

    def look_up(block, carry):
        rows = pl.ds(pl.multiple_of(block * 8, 8), 8)
        for side in range(2):
            at = index[rows, side * LANES : (side + 1) * LANES]
            low, level_of = at & (LANES - 1), at >> 7
            width = min(LANES, TOK - side * LANES)
            for h in range(heads):
                total = jnp.zeros((8, LANES), F32)
                for level in range(levels):
                    source = jnp.broadcast_to(
                        table[h : h + 1, level * LANES : (level + 1) * LANES], (8, LANES))
                    found = jnp.take_along_axis(source, low, axis=1, mode="promise_in_bounds")
                    total = jnp.where(level_of == level, found, total)
                bias[h, rows, side * LANES : side * LANES + width] = total[:, :width]
        return carry

    lax.fori_loop(0, TOK // 8, look_up, 0)

    lat = lax.axis_index("lat")
    grid_row = lat * height + lax.broadcasted_iota(jnp.int32, (height, breadth), 0)
    wrapped = (grid_row >= height * lax.axis_size("lat") - SHIFT).astype(jnp.int32)
    labels[...] = (region_ref[...] * 2 + wrapped).astype(F32)

    yield
    x_normed, x_inverse = normalize(x_ref[...])
    put(xn_s, slice(None), x_normed)
    spread[0] = jnp.broadcast_to(x_inverse, (tokens, LANES))
    qkv = dot_nn(pair(xn_s), pair(wq))
    q = qkv[:, :D] * SCALE
    q_s[...] = q
    for j, part in enumerate((q, qkv[:, D : 2 * D], qkv[:, 2 * D :])):
        upper, lower = split(part)
        qkv_s[0, :, j * D : (j + 1) * D] = upper
        qkv_s[1, :, j * D : (j + 1) * D] = lower

    lane_head = lax.broadcasted_iota(jnp.int32, (TOK, LANES), 1) >> 5

    def only(head, values):
        keep = lane_head == head
        return tuple(jnp.where(keep, v, jnp.zeros_like(v)) for v in values)

    def tile(which, t, rows):
        cols = slice(which * D + t * LANES, which * D + (t + 1) * LANES)
        return qkv_s[0, rows, cols], qkv_s[1, rows, cols]

    def forward(w, carry):
        rows = pl.ds(pl.multiple_of(w * TOK, TOK), TOK)
        first_row, first_col = (w // across) * WIN, (w % across) * WIN
        position = lax.broadcasted_iota(jnp.int32, (TOK, height), 0)
        quotient = (position * 171) >> 11
        hot = (lax.broadcasted_iota(jnp.int32, (TOK, height), 1) == quotient + first_row).astype(F32)
        picked = mul(hot.astype(BF16), labels[...].astype(BF16), NN)
        position = lax.broadcasted_iota(jnp.int32, (TOK, breadth), 0)
        rest = position - WIN * ((position * 171) >> 11)
        chosen = lax.broadcasted_iota(jnp.int32, (TOK, breadth), 1) == rest + first_col
        label = jnp.sum(jnp.where(chosen, picked, 0.0), axis=1, keepdims=True)
        across_label = jnp.transpose(jnp.broadcast_to(label, (TOK, LANES)))[:1]
        allowed = label == across_label
        for t in range(D // LANES):
            q, k, v = (tile(j, t, rows) for j in range(3))
            total = jnp.zeros((TOK, LANES), F32)
            for head in range(PACK):
                h = t * PACK + head
                scores = dot_nt(only(head, q), k) + bias[h]
                masked = jnp.where(allowed, scores, -jnp.inf)
                raised = jnp.exp(masked - jnp.max(masked, axis=-1, keepdims=True))
                p = split(raised * (1.0 / jnp.sum(raised, axis=-1, keepdims=True)))
                prob[0, w * heads + h], prob[1, w * heads + h] = p
                total += dot_cols(p, only(head, v))
            ctx_s[rows, t * LANES : (t + 1) * LANES] = total
        return carry

    lax.fori_loop(0, count, forward, 0)

    mixed = x_ref[...] + dot_nn(split(ctx_s[...]), pair(wp))
    yield
    put(ct_s, slice(None), ct_ref[...])
    m_normed, m_inverse = normalize(mixed)
    put(mn_s, slice(None), m_normed)
    spread[1] = jnp.broadcast_to(m_inverse, (tokens, LANES))
    for n, value in enumerate((m_normed, ct_ref[...])):
        turned[n, 0], turned[n, 1] = split(jnp.transpose(value))
    acc[...] = jnp.zeros_like(acc)

    def feed(f, carry):
        cols = pl.ds(pl.multiple_of(f * FF_BLOCK, FF_BLOCK), FF_BLOCK)
        w_up = pair(wu, slice(None), cols)
        hidden, slope = gelu_and_slope(dot_nn(pair(mn_s), w_up))
        d_up = split(dot_nt(pair(ct_s), pair(wd, cols)) * slope)
        hidden = split(hidden)
        blocks = FF // LANES
        grad = dot_rows((turned[0, 0], turned[0, 1]), d_up)
        for j in range(FF_BLOCK // LANES):
            start = row_of[2] + f * (FF_BLOCK // LANES) + j
            grad_ref[pl.ds(start, D, stride=blocks), :] = grad[:, j * LANES : (j + 1) * LANES]
        grad = jnp.transpose(dot_rows((turned[1, 0], turned[1, 1]), hidden))
        blocks = D // LANES
        for j in range(blocks):
            start = row_of[3] + f * (FF_BLOCK * blocks) + j
            grad_ref[pl.ds(start, FF_BLOCK, stride=blocks), :] = grad[:, j * LANES : (j + 1) * LANES]
        acc[...] += dot_nt(d_up, w_up)
        return carry

    lax.fori_loop(0, FF // FF_BLOCK, feed, 0)

    d_mixed = ct_ref[...] + normalize_backward(acc[...], full(mn_s), spread[1][:, :1])
    acc[...] = d_mixed
    d_pair = split(d_mixed)
    turned[0, 0], turned[0, 1] = split(jnp.transpose(ctx_s[...]))
    grad = dot_rows((turned[0, 0], turned[0, 1]), d_pair)
    blocks = D // LANES
    for j in range(blocks):
        grad_ref[pl.ds(row_of[1] + j, D, stride=blocks), :] = grad[:, j * LANES : (j + 1) * LANES]
    d_s[...] = dot_nt(d_pair, pair(wp))
    dbias[...] = jnp.zeros_like(dbias)

    def backward(w, carry):
        rows = pl.ds(pl.multiple_of(w * TOK, TOK), TOK)
        for t in range(D // LANES):
            cols = slice(t * LANES, (t + 1) * LANES)
            k, v = tile(1, t, rows), tile(2, t, rows)
            grad = d_s[rows, cols]
            weighed = grad * ctx_s[rows, cols]
            g = split(grad)
            g_turned = split(jnp.transpose(grad))
            q_turned = split(jnp.transpose(q_s[rows, cols]))
            dq = jnp.zeros((TOK, LANES), F32)
            dk, dv = [], []
            for head in range(PACK):
                h = t * PACK + head
                part = slice(head * HEAD_DIM, (head + 1) * HEAD_DIM)
                upper, lower = prob[0, w * heads + h], prob[1, w * heads + h]
                dprob = dot_nt(only(head, g), v)
                delta = jnp.sum(jnp.where(lane_head == head, weighed, 0.0), axis=-1, keepdims=True)
                dscore = (upper.astype(F32) + lower.astype(F32)) * (dprob - delta)
                dbias[h] += dscore
                ds = split(dscore)
                dq += dot_cols(ds, only(head, k))
                dk.append(dot_rows((q_turned[0][part], q_turned[1][part]), ds))
                dv.append(dot_rows((g_turned[0][part], g_turned[1][part]), (upper, lower)))
            for j, value in enumerate((dq * SCALE, jnp.transpose(jnp.concatenate(dk, 0)),
                                       jnp.transpose(jnp.concatenate(dv, 0)))):
                at = slice(j * D + t * LANES, j * D + (t + 1) * LANES)
                upper, lower = split(value)
                dqkv_s[0, rows, at], dqkv_s[1, rows, at] = upper, lower
        return carry

    lax.fori_loop(0, count, backward, 0)

    x_normed = full(xn_s)
    turned[1, 0], turned[1, 1] = split(jnp.transpose(x_normed))
    grad = dot_rows((turned[1, 0], turned[1, 1]), pair(dqkv_s))
    blocks = 3 * D // LANES
    for j in range(blocks):
        grad_ref[pl.ds(row_of[0] + j, D, stride=blocks), :] = grad[:, j * LANES : (j + 1) * LANES]
    yield
    d_normed = dot_nt(pair(dqkv_s), pair(wq))
    yield
    q_s[...] = acc[...] + normalize_backward(d_normed, x_normed, spread[0][:, :1])
    edge_ref[...] = jnp.zeros_like(edge_ref)
    for at, row, col in window_pieces(height, breadth):
        edge_ref[row, col : col + WIN] = q_s[at : at + WIN]

    yield
    table_acc = jnp.zeros((levels * 2 * HEAD_ROWS, LANES), F32)

    def collect(block, total):
        rows = pl.ds(pl.multiple_of(block * 8, 8), 8)
        at_rows = index_ref[rows, :]
        grads = dbias[:, rows, :]
        for r in range(8):
            at = at_rows[r : r + 1]
            low, level_of = at & (LANES - 1), at >> 7
            grad = jnp.concatenate([grads[:, r, :], jnp.zeros((HEAD_ROWS - heads, TOK), F32)], 0)
            stacked = jnp.concatenate(
                [jnp.where(level_of == level, grad, 0.0) for level in range(levels)], 0)
            hot = (lax.broadcasted_iota(jnp.int32, (LANES, TOK), 0) == low).astype(F32).astype(BF16)
            total = total + mul(jnp.concatenate(split(stacked), 0), hot, NT)
        return total

    total = lax.fori_loop(0, TOK // 8, collect, table_acc)
    table_out[...] = total[: levels * HEAD_ROWS] + total[levels * HEAD_ROWS :]


def block_kernel(*refs):
    for _ in block_steps(*refs):
        pass


def block_scratch(tokens, height, breadth, heads, entries):
    levels = -(-entries // LANES)
    return [
        pltpu.VMEM((2, D, 3 * D), BF16),
        pltpu.VMEM((2, D, D), BF16),
        pltpu.VMEM((2, D, FF), BF16),
        pltpu.VMEM((2, FF, D), BF16),
        pltpu.VMEM((HEAD_ROWS, levels * LANES), F32),
        pltpu.VMEM((TOK, 2 * LANES), jnp.int32),
        pltpu.VMEM((heads, TOK, TOK), F32),
        pltpu.VMEM((2, tokens // TOK * heads, TOK, TOK), BF16),
        pltpu.VMEM((2, tokens, D), BF16),
        pltpu.VMEM((2, tokens, D), BF16),
        pltpu.VMEM((2, tokens, D), BF16),
        pltpu.VMEM((2, tokens, 3 * D), BF16),
        pltpu.VMEM((tokens, D), F32),
        pltpu.VMEM((tokens, D), F32),
        pltpu.VMEM((2, 2, D, tokens), BF16),
        pltpu.VMEM((tokens, D), F32),
        pltpu.VMEM((height, breadth), F32),
        pltpu.VMEM((2, tokens, LANES), F32),
    ]


def table_rows(entries):
    return -(-entries // LANES) * HEAD_ROWS


def block_gradients(x, ct, weights, bias_table, bias_index, region_ids):
    tokens = x.shape[0]
    height, breadth = region_ids.shape
    heads, entries = bias_table.shape
    vmem = pl.BlockSpec(memory_space=pltpu.VMEM)
    return pl.pallas_call(
        block_kernel,
        in_specs=[vmem] * 6,
        out_specs=[vmem] * 3,
        out_shape=[
            jax.ShapeDtypeStruct((weights.shape[0] // LANES, LANES), F32),
            jax.ShapeDtypeStruct((height + SHIFT, breadth + EDGE, D), F32),
            jax.ShapeDtypeStruct((table_rows(entries), LANES), F32),
        ],
        scratch_shapes=[pltpu.VMEM((tokens, D), F32)]
        + block_scratch(tokens, height, breadth, heads, entries),
        compiler_params=pltpu.CompilerParams(vmem_limit_bytes=VMEM_LIMIT),
    )(x, ct, weights.reshape(-1, LANES), bias_table, bias_index, region_ids)


def bit_count(size):
    return size.bit_length() - 1


def bit_partners(lat_bits, lon_bits):
    bits = lat_bits + lon_bits
    lat, lon = lax.axis_index("lat"), lax.axis_index("lon")
    mine, partner = [], []
    for b in range(bits):
        if b < lat_bits:
            step = 1 << (lat_bits - 1 - b)
            bit = lax.rem(lat // step, 2)
            partner.append({"lat": lat + step * (1 - 2 * bit), "lon": lon})
        else:
            step = 1 << (bits - 1 - b)
            bit = lax.rem(lon // step, 2)
            partner.append({"lat": lat, "lon": lon + step * (1 - 2 * bit)})
        mine.append(bit)
    return mine, partner


def exchange_steps(lat_bits, lon_bits, chunks, factor, grad_ref, table_ref, edge_ref, weight_ref,
                   first_ref, second_ref, new_ref, first_out, second_out, table_final, dx_out, *scratch):
    bits = lat_bits + lon_bits
    mine, partner = bit_partners(lat_bits, lon_bits)
    core, inner = bits - 1, list(range(lat_bits, bits - 1))[::-1]
    ahead, back = list(range(lat_bits))[::-1], list(range(lat_bits))
    orders = [[core] + (ahead if i % 2 == 0 else back) + inner for i in range(len(chunks))]
    orders[-1] = [core] + inner + ahead
    held = [scratch[i * bits : (i + 1) * bits] for i in range(len(chunks))]
    table_held, table_out = scratch[len(chunks) * bits : len(chunks) * bits + 2]
    west_in, north_in, corner_in, own_weight, rs_send, rs_recv, ag_send, ag_recv, t_send, t_recv, e_send, e_recv, w_sem = scratch[
        len(chunks) * bits + 2 :
    ]

    height, breadth, _ = dx_out.shape
    edges = [
        pltpu.make_async_remote_copy(
            src_ref=src, dst_ref=dst, send_sem=e_send.at[n], recv_sem=e_recv.at[n],
            device_id=where, device_id_type=pl.DeviceIdType.MESH)
        for n, (src, dst, where) in enumerate(zip(
            (edge_ref.at[pl.ds(SHIFT, height - SHIFT), pl.ds(breadth, EDGE)],
             edge_ref.at[pl.ds(height, SHIFT), pl.ds(0, breadth)],
             edge_ref.at[pl.ds(height, SHIFT), pl.ds(breadth, EDGE)]),
            (west_in, north_in, corner_in), neighbours(1)))
    ]

    def copy(src, dst, send, recv, b):
        return pltpu.make_async_remote_copy(
            src_ref=src, dst_ref=dst, send_sem=send, recv_sem=recv,
            device_id=partner[b], device_id_type=pl.DeviceIdType.MESH)

    def select(dims, b, value):
        return tuple(value if d == b else slice(None) for d in dims)

    def reduce_copy(i, s):
        order, (start, rows) = orders[i], chunks[i]
        b = order[s]
        dims = sorted(order[s:])
        if s == 0:
            src = grad_ref.at[select(dims, b, 1 - mine[b]) + (pl.ds(start, rows),)]
        else:
            src = held[i][s - 1].at[select(dims, b, 1 - mine[b])]
        return copy(src, held[i][s], rs_send.at[i, s], rs_recv.at[i, s], b)

    def reduce_add(i, s):
        order, (start, rows) = orders[i], chunks[i]
        b = order[s]
        dims = sorted(order[s:])
        if s == 0:
            kept = grad_ref[select(dims, b, mine[b]) + (pl.ds(start, rows),)]
        else:
            kept = held[i][s - 1][select(dims, b, mine[b])]
        held[i][s][...] += kept

    def gather_copy(i, s):
        order, (start, rows) = orders[i], chunks[i]
        known = set(order[s + 1 :])
        index = tuple(slice(None) if d in known else mine[d] for d in range(bits))
        region = new_ref.at[index + (pl.ds(start, rows),)]
        return copy(region, region, ag_send.at[i, s], ag_recv.at[i, s], order[s])

    def table_copy(s):
        return copy(table_out if s else table_ref, table_held.at[s], t_send.at[s], t_recv.at[s], orders[0][s])

    fetch = pltpu.make_async_copy(weight_ref.at[tuple(mine)], own_weight, w_sem)
    fetch.start()
    n = len(chunks)
    live = {}
    for i in range(n):
        live[i] = reduce_copy(i, 0)
        live[i].start()
    yield
    for s in range(bits):
        for i in range(n):
            live[i].wait()
            reduce_add(i, s)
            if s + 1 < bits:
                live[i] = reduce_copy(i, s + 1)
                live[i].start()
            else:
                if i == 0:
                    fetch.wait()
                rows = pl.ds(*chunks[i])
                grad = held[i][s][...] * factor
                first = 0.9 * first_ref[rows] + 0.1 * grad
                second = 0.95 * second_ref[rows] + 0.05 * grad * grad
                first_out[rows] = first
                second_out[rows] = second
                new_ref[tuple(mine) + (rows,)] = own_weight[rows] - 0.01 * first / (jnp.sqrt(second) + 1e-08)
                live[i] = gather_copy(i, s)
                live[i].start()
        if s == 0:
            yield
            for edge in edges:
                edge.start()
            yield
            table_live = table_copy(0)
            table_live.start()
        table_live.wait()
        if s == 0:
            table_out[...] = table_ref[...] + table_held[s]
        else:
            table_out[...] += table_held[s]
        if s + 1 < bits:
            table_live = table_copy(s + 1)
            table_live.start()
    heads, entries = table_final.shape
    for level in range(-(-entries // LANES)):
        width = min(LANES, entries - level * LANES)
        table_final[:, pl.ds(level * LANES, width)] = (
            table_out[pl.ds(level * HEAD_ROWS, heads), pl.ds(0, width)] * factor
        )
    for edge in edges:
        edge.wait()
    dx_out[SHIFT:, EDGE:] = edge_ref[SHIFT:height, EDGE:breadth]
    dx_out[:SHIFT, EDGE:] = north_in[:, EDGE:]
    column = lax.broadcasted_iota(jnp.int32, (1, EDGE, D), 1)
    dx_out[SHIFT:, :EDGE] = jnp.where(column < SHIFT, west_in[...], edge_ref[SHIFT:height, :EDGE])
    dx_out[:SHIFT, :EDGE] = jnp.where(column < SHIFT, corner_in[...], north_in[:, :EDGE])
    for s in reversed(range(bits)):
        for i in range(n):
            live[i].wait()
            if s > 0:
                live[i] = gather_copy(i, s - 1)
                live[i].start()


def exchange_kernel(lat_bits, lon_bits, *refs):
    greet(bit_partners(lat_bits, lon_bits)[1] + list(neighbours(-1)))
    for _ in exchange_steps(lat_bits, lon_bits, *refs):
        pass


def chunk_rows(rows, count):
    groups = -(-rows // 8)
    edges = [min(8 * (groups * i // count), rows) for i in range(count)] + [rows]
    return [(a, b - a) for a, b in zip(edges, edges[1:])]


def exchange_scratch(bits, chunks, rows, table_shape, tile_shape):
    height, breadth, _ = tile_shape
    dma = pltpu.SemaphoreType.DMA
    return [
        pltpu.VMEM((2,) * (bits - 1 - s) + (count, LANES), F32)
        for _, count in chunks
        for s in range(bits)
    ] + [
        pltpu.VMEM((bits,) + table_shape, F32),
        pltpu.VMEM(table_shape, F32),
        pltpu.VMEM((height - SHIFT, EDGE, D), F32),
        pltpu.VMEM((SHIFT, breadth, D), F32),
        pltpu.VMEM((SHIFT, EDGE, D), F32),
        pltpu.VMEM((rows, LANES), F32),
        dma((len(chunks), bits)), dma((len(chunks), bits)),
        dma((len(chunks), bits)), dma((len(chunks), bits)),
        dma((bits,)), dma((bits,)), dma((3,)), dma((3,)), dma(()),
    ]


def fused_kernel(lat_bits, lon_bits, chunks, factor, n_exchange, x_hbm, ct_hbm, weight_ref, table_ref,
                 index_ref, region_ref, first_ref, second_ref, new_ref, first_out, second_out,
                 table_final, dx_out, grad, table_part, xw, ctw, wide, send, recv, local, w_sem, *scratch):
    greet(bit_partners(lat_bits, lon_bits)[1] + list(neighbours(1)) + list(neighbours(-1)))
    staged = pltpu.make_async_copy(weight_ref, new_ref, w_sem)
    staged.start()
    copies = [halo_copies(n, ref, wide, send, recv, local) for n, ref in enumerate((x_hbm, ct_hbm))]
    edge = wide.at[0]
    block = block_steps(xw, ctw, new_ref.reshape(grad.shape), table_ref, index_ref, region_ref, grad,
                        edge, table_part, xw, *scratch[n_exchange:])
    exchange = exchange_steps(lat_bits, lon_bits, chunks, factor, grad.reshape(new_ref.shape), table_part,
                              edge, weight_ref, first_ref, second_ref, new_ref, first_out, second_out,
                              table_final, dx_out, *scratch[:n_exchange])
    next(block)
    staged.wait()
    next(block)
    assemble(0, copies[0], x_hbm.shape, wide, xw)
    next(block)
    assemble(1, copies[1], x_hbm.shape, wide, ctw)
    next(block)
    next(exchange)
    next(block)
    next(exchange)
    next(block)
    next(exchange)
    for _ in block:
        pass
    for _ in exchange:
        pass


def whole_step(block_input, cotangent, weights, first, second, bias_table, bias_index, region_ids, factor):
    lat_bits, lon_bits = bit_count(lax.axis_size("lat")), bit_count(lax.axis_size("lon"))
    bits = lat_bits + lon_bits
    rows = first.shape[0] // LANES
    chunks = chunk_rows(rows, CHUNKS)
    split_shape = (2,) * bits + (rows, LANES)
    tile_shape = block_input.shape
    height, breadth, _ = tile_shape
    tokens = height * breadth
    heads, entries = bias_table.shape
    table_shape = (table_rows(entries), LANES)
    vmem, anywhere = pl.BlockSpec(memory_space=pltpu.VMEM), pl.BlockSpec(memory_space=pl.ANY)
    shard = jax.ShapeDtypeStruct((rows, LANES), F32)
    dma = pltpu.SemaphoreType.DMA
    for_exchange = exchange_scratch(bits, chunks, rows, table_shape, tile_shape)
    new, first_new, second_new, table_sum, dx = pl.pallas_call(
        functools.partial(fused_kernel, lat_bits, lon_bits, chunks, factor, len(for_exchange)),
        in_specs=[anywhere] * 3 + [vmem] * 5,
        out_specs=[vmem] * 5,
        out_shape=[jax.ShapeDtypeStruct(split_shape, F32), shard, shard,
                   jax.ShapeDtypeStruct(bias_table.shape, F32),
                   jax.ShapeDtypeStruct(tile_shape, F32)],
        scratch_shapes=[
            pltpu.VMEM((weights.shape[0] // LANES, LANES), F32),
            pltpu.VMEM(table_shape, F32),
            pltpu.VMEM((tokens, D), F32),
            pltpu.VMEM((tokens, D), F32),
            pltpu.VMEM((2, height + SHIFT, breadth + EDGE, D), F32),
            dma((2, 3)), dma((2, 3)), dma((2,)), dma(()),
        ] + for_exchange + block_scratch(tokens, height, breadth, heads, entries),
        compiler_params=pltpu.CompilerParams(
            collective_id=2, has_side_effects=True, vmem_limit_bytes=VMEM_LIMIT),
    )(block_input, cotangent, weights.reshape(split_shape), bias_table, bias_index, region_ids,
      first.reshape(rows, LANES), second.reshape(rows, LANES))
    return new.reshape(-1), first_new.reshape(-1), second_new.reshape(-1), table_sum, dx


def reduce_update_gather(grads, table, edge, weights, first, second, table_shape, tile_shape, factor):
    lat_bits, lon_bits = bit_count(lax.axis_size("lat")), bit_count(lax.axis_size("lon"))
    bits = lat_bits + lon_bits
    rows = first.shape[0] // LANES
    chunks = chunk_rows(rows, CHUNKS)
    split_shape = (2,) * bits + (rows, LANES)
    vmem = pl.BlockSpec(memory_space=pltpu.VMEM)
    shard = jax.ShapeDtypeStruct((rows, LANES), F32)
    new, first_new, second_new, table_sum, dx = pl.pallas_call(
        functools.partial(exchange_kernel, lat_bits, lon_bits, chunks, factor),
        in_specs=[vmem, vmem, vmem, pl.BlockSpec(memory_space=pl.ANY), vmem, vmem],
        out_specs=[vmem] * 5,
        out_shape=[jax.ShapeDtypeStruct(split_shape, F32), shard, shard,
                   jax.ShapeDtypeStruct(table_shape, F32),
                   jax.ShapeDtypeStruct(tile_shape, F32)],
        scratch_shapes=exchange_scratch(bits, chunks, rows, table.shape, tile_shape),
        compiler_params=pltpu.CompilerParams(
            collective_id=0, has_side_effects=True, vmem_limit_bytes=56 * 1024 * 1024),
    )(grads.reshape(split_shape), table, edge, weights.reshape(split_shape),
      first.reshape(rows, LANES), second.reshape(rows, LANES))
    return new.reshape(-1), first_new.reshape(-1), second_new.reshape(-1), table_sum, dx


def per_device(
    block_input, cotangent, weights, first_moment, second_moment, bias_table, bias_index, region_ids
):
    tile_rows, tile_cols, _ = block_input.shape
    devices = lax.axis_size("lat") * lax.axis_size("lon")
    factor = 1.0 / math.sqrt(tile_rows * tile_cols * devices)
    if first_moment.shape[0] % (8 * LANES) == 0:
        gathered, first_new, second_new, table_grad, grad_input = whole_step(
            block_input, cotangent, weights, first_moment, second_moment, bias_table, bias_index,
            region_ids, factor,
        )
        return (grad_input, gathered, first_new, second_new, table_grad)
    x, ct = gather_windows(block_input, cotangent)
    grads, edge, table = block_gradients(x, ct, weights, bias_table, bias_index, region_ids)
    gathered, first_new, second_new, table_grad, grad_input = reduce_update_gather(
        grads, table, edge, weights, first_moment, second_moment, bias_table.shape,
        block_input.shape, factor,
    )
    return (grad_input, gathered, first_new, second_new, table_grad)


def solution(mesh):
    placed = (
        P("lat", "lon", None),
        P("lat", "lon", None),
        P(),
        P(("lat", "lon")),
        P(("lat", "lon")),
        P(),
        P(),
        P("lat", "lon"),
    )
    return jax.shard_map(
        per_device,
        mesh=mesh,
        in_specs=placed,
        out_specs=(P("lat", "lon", None), P(), P(("lat", "lon")), P(("lat", "lon")), P()),
        check_vma=False,
    )
```

```python
import functools
import math

import jax
import jax.numpy as jnp
from jax import lax
from jax.experimental import pallas as pl
from jax.experimental.pallas import tpu as pltpu
from jax.sharding import PartitionSpec as P

D = 384
HEADS = 12
FF = 1536
WIN = 12
HEAD_DIM = 32
SHIFT = 6
TOK = WIN * WIN
HEAD_ROWS = 16
LANES = 128
PACK = LANES // HEAD_DIM
EDGE = 8
FF_BLOCK = 512
CHUNKS = 5
SEGMENT = 2
PACE = (0, 2, 2, 2, 3, 3)
LATER = (3, 3)
SCALE = 1.0 / math.sqrt(HEAD_DIM)

F32 = jnp.float32
BF16 = jnp.bfloat16
NN = (((1,), (0,)), ((), ()))
NT = (((1,), (1,)), ((), ()))
VMEM_LIMIT = 63 * 1024 * 1024

def neighbours(by):
    lat_size, lon_size = lax.axis_size("lat"), lax.axis_size("lon")
    lat = lax.rem(lax.axis_index("lat") + by + lat_size, lat_size)
    lon = lax.rem(lax.axis_index("lon") + by + lon_size, lon_size)
    return ({"lon": lon}, {"lat": lat}, {"lat": lat, "lon": lon})


def split(value):
    upper = value.astype(BF16)
    return upper, (value - upper.astype(F32)).astype(BF16)


def mul(a, b, dims):
    return lax.dot_general(a, b, dims, preferred_element_type=F32)


def dot_nn(a, b):
    return mul(jnp.concatenate([a[0], a[0], a[1]], 1), jnp.concatenate([b[0], b[1], b[0]], 0), NN)


def dot_nt(a, b):
    return mul(jnp.concatenate([a[0], a[0], a[1]], 1), jnp.concatenate([b[0], b[1], b[0]], 1), NT)


def dot_rows(a, b):
    rows = a[0].shape[0]
    both = mul(jnp.concatenate([a[0], a[1]], 0), b[0], NN)
    return both[:rows] + both[rows:] + mul(a[0], b[1], NN)


def dot_cols(a, b):
    cols = b[0].shape[1]
    both = mul(a[0], jnp.concatenate([b[0], b[1]], 1), NN)
    return both[:, :cols] + both[:, cols:] + mul(a[1], b[0], NN)


def normalize(values):
    center = values - jnp.mean(values, axis=-1, keepdims=True)
    spread = jnp.mean(center * center, axis=-1, keepdims=True)
    inverse = 1.0 / jnp.sqrt(spread + 1e-05)
    return center * inverse, inverse


def normalize_backward(grad, normed, inverse):
    return inverse * (
        grad
        - jnp.mean(grad, axis=-1, keepdims=True)
        - normed * jnp.mean(grad * normed, axis=-1, keepdims=True)
    )


def gelu_and_slope(u):
    c = math.sqrt(2.0 / math.pi)
    square = u * u
    t = jnp.tanh(c * u * (1.0 + 0.044715 * square))
    half = 0.5 * (1.0 + t)
    slope = half + 0.5 * u * (1.0 - t * t) * (c * (1.0 + 3.0 * 0.044715 * square))
    return u * half, slope


def window_pieces(height, breadth):
    at = 0
    for r in range(height // WIN):
        for c in range(breadth // WIN):
            for i in range(WIN):
                yield at, SHIFT + r * WIN + i, SHIFT + c * WIN
                at += WIN


def greet(places):
    barrier = pltpu.get_barrier_semaphore()
    for where in places:
        pl.semaphore_signal(barrier, inc=1, device_id=where, device_id_type=pl.DeviceIdType.MESH)
    pl.semaphore_wait(barrier, len(places))


def halo_copies(n, ref, wide, send, recv, local):
    height, breadth, _ = ref.shape
    parts = (
        (ref.at[:, pl.ds(0, EDGE)], wide.at[n, pl.ds(0, height), pl.ds(breadth, EDGE)]),
        (ref.at[pl.ds(0, SHIFT)], wide.at[n, pl.ds(height, SHIFT), pl.ds(0, breadth)]),
        (ref.at[pl.ds(0, SHIFT), pl.ds(0, EDGE)],
         wide.at[n, pl.ds(height, SHIFT), pl.ds(breadth, EDGE)]),
    )
    copies = [
        pltpu.make_async_remote_copy(
            src_ref=src, dst_ref=dst, send_sem=send.at[n, k], recv_sem=recv.at[n, k],
            device_id=where, device_id_type=pl.DeviceIdType.MESH)
        for k, ((src, dst), where) in enumerate(zip(parts, neighbours(-1)))
    ]
    copies.append(pltpu.make_async_copy(
        ref, wide.at[n, pl.ds(0, height), pl.ds(0, breadth)], local.at[n]))
    for copy in copies:
        copy.start()
    return copies


def assemble(n, copies, shape, wide, out):
    for copy in copies:
        copy.wait()
    for at, row, col in window_pieces(shape[0], shape[1]):
        out[at : at + WIN] = wide[n, row, col : col + WIN]


def halo_kernel(x_ref, ct_ref, xw_ref, ctw_ref, wide, send, recv, local):
    greet(neighbours(1))
    copies = [halo_copies(n, ref, wide, send, recv, local) for n, ref in enumerate((x_ref, ct_ref))]
    for n, out in enumerate((xw_ref, ctw_ref)):
        assemble(n, copies[n], x_ref.shape, wide, out)


def gather_windows(block_input, cotangent):
    height, breadth, _ = block_input.shape
    dma = pltpu.SemaphoreType.DMA
    return pl.pallas_call(
        halo_kernel,
        in_specs=[pl.BlockSpec(memory_space=pl.ANY)] * 2,
        out_specs=[pl.BlockSpec(memory_space=pltpu.VMEM)] * 2,
        out_shape=[jax.ShapeDtypeStruct((height * breadth, D), F32)] * 2,
        scratch_shapes=[
            pltpu.VMEM((2, height + SHIFT, breadth + EDGE, D), F32),
            dma((2, 3)), dma((2, 3)), dma((2,)),
        ],
        compiler_params=pltpu.CompilerParams(collective_id=1, has_side_effects=True),
    )(block_input, cotangent)


def block_steps(x_ref, ct_ref, w_ref, table_ref, index_ref, region_ref, grad_ref, edge_ref,
                table_out, d_s, wq, wp, wu, wd, table, index, bias, prob, xn_s, mn_s, ct_s,
                qkv_s, q_s, ctx_s, turned, acc, labels, spread):
    dbias, dqkv_s = bias, qkv_s
    height, breadth = region_ref.shape
    across = breadth // WIN
    tokens = x_ref.shape[0]
    count = tokens // TOK
    heads, entries = table_ref.shape
    levels = table.shape[1] // LANES
    row_of = [0, D * 3 * D // LANES, (D * 3 * D + D * D) // LANES, (D * 3 * D + D * D + D * FF) // LANES]

    def put(ref, rows, value):
        upper, lower = split(value)
        ref[0, rows], ref[1, rows] = upper, lower

    def put_turned(n, value):
        upper, lower = split(jnp.transpose(value))
        for j, part in enumerate((upper, upper, lower)):
            turned[n, :, j * tokens : (j + 1) * tokens] = part

    def weight_grad(n, b):
        return mul(turned[n], jnp.concatenate([b[0], b[1], b[0]], 0), NN)

    def pair(ref, *at):
        return ref[(0,) + at], ref[(1,) + at]

    def full(ref):
        return ref[0].astype(F32) + ref[1].astype(F32)

    yield
    for dst, start in zip((wq, wp, wu, wd), row_of):
        _, rows, width = dst.shape
        blocks = width // LANES
        for j in range(blocks):
            upper, lower = split(w_ref[pl.ds(start + j, rows, stride=blocks), :])
            dst[0, :, j * LANES : (j + 1) * LANES] = upper
            dst[1, :, j * LANES : (j + 1) * LANES] = lower

    table[...] = jnp.zeros_like(table)
    table[:heads, :entries] = table_ref[...]
    index[...] = jnp.zeros_like(index)
    index[:, :TOK] = index_ref[...]

    def look_up(block, carry):
        rows = pl.ds(pl.multiple_of(block * 8, 8), 8)
        for side in range(2):
            at = index[rows, side * LANES : (side + 1) * LANES]
            low, level_of = at & (LANES - 1), at >> 7
            width = min(LANES, TOK - side * LANES)
            for h in range(heads):
                total = jnp.zeros((8, LANES), F32)
                for level in range(levels):
                    source = jnp.broadcast_to(
                        table[h : h + 1, level * LANES : (level + 1) * LANES], (8, LANES))
                    found = jnp.take_along_axis(source, low, axis=1, mode="promise_in_bounds")
                    total = jnp.where(level_of == level, found, total)
                bias[h, rows, side * LANES : side * LANES + width] = total[:, :width]
        return carry

    lax.fori_loop(0, TOK // 8, look_up, 0)

    lat = lax.axis_index("lat")
    grid_row = lat * height + lax.broadcasted_iota(jnp.int32, (height, breadth), 0)
    wrapped = (grid_row >= height * lax.axis_size("lat") - SHIFT).astype(jnp.int32)
    labels[...] = (region_ref[...] * 2 + wrapped).astype(F32)

    yield
    x_normed, x_inverse = normalize(x_ref[...])
    put(xn_s, slice(None), x_normed)
    spread[0] = jnp.broadcast_to(x_inverse, (tokens, LANES))
    qkv = dot_nn(pair(xn_s), pair(wq))
    q = qkv[:, :D] * SCALE
    q_s[...] = q
    for j, part in enumerate((q, qkv[:, D : 2 * D], qkv[:, 2 * D :])):
        upper, lower = split(part)
        qkv_s[0, :, j * D : (j + 1) * D] = upper
        qkv_s[1, :, j * D : (j + 1) * D] = lower

    lane_head = lax.broadcasted_iota(jnp.int32, (TOK, LANES), 1) >> 5

    def only(head, values):
        keep = lane_head == head
        return tuple(jnp.where(keep, v, jnp.zeros_like(v)) for v in values)

    def tile(which, t, rows):
        cols = pl.ds(pl.multiple_of(which * D + t * LANES, LANES), LANES)
        return qkv_s[0, rows, cols], qkv_s[1, rows, cols]

    def forward(w, carry):
        rows = pl.ds(pl.multiple_of(w * TOK, TOK), TOK)
        first_row, first_col = (w // across) * WIN, (w % across) * WIN
        position = lax.broadcasted_iota(jnp.int32, (TOK, height), 0)
        quotient = (position * 171) >> 11
        hot = (lax.broadcasted_iota(jnp.int32, (TOK, height), 1) == quotient + first_row).astype(F32)
        picked = mul(hot.astype(BF16), labels[...].astype(BF16), NN)
        position = lax.broadcasted_iota(jnp.int32, (TOK, breadth), 0)
        rest = position - WIN * ((position * 171) >> 11)
        chosen = lax.broadcasted_iota(jnp.int32, (TOK, breadth), 1) == rest + first_col
        label = jnp.sum(jnp.where(chosen, picked, 0.0), axis=1, keepdims=True)
        across_label = jnp.transpose(jnp.broadcast_to(label, (TOK, LANES)))[:1]
        allowed = label == across_label
        for t in range(D // LANES):
            q, k, v = (tile(j, t, rows) for j in range(3))
            total = jnp.zeros((TOK, LANES), F32)
            for head in range(PACK):
                h = t * PACK + head
                scores = dot_nt(only(head, q), k) + bias[h]
                masked = jnp.where(allowed, scores, -jnp.inf)
                raised = jnp.exp(masked - jnp.max(masked, axis=-1, keepdims=True))
                p = split(raised * (1.0 / jnp.sum(raised, axis=-1, keepdims=True)))
                prob[0, w * heads + h], prob[1, w * heads + h] = p
                total += dot_cols(p, only(head, v))
            ctx_s[rows, t * LANES : (t + 1) * LANES] = total
        return carry

    lax.fori_loop(0, count, forward, 0)

    mixed = x_ref[...] + dot_nn(split(ctx_s[...]), pair(wp))
    yield
    put(ct_s, slice(None), ct_ref[...])
    m_normed, m_inverse = normalize(mixed)
    put(mn_s, slice(None), m_normed)
    spread[1] = jnp.broadcast_to(m_inverse, (tokens, LANES))
    for n, value in enumerate((m_normed, ct_ref[...])):
        put_turned(n, value)
    acc[...] = jnp.zeros_like(acc)

    def feed(f, carry):
        cols = pl.ds(pl.multiple_of(f * FF_BLOCK, FF_BLOCK), FF_BLOCK)
        w_up = pair(wu, slice(None), cols)
        hidden, slope = gelu_and_slope(dot_nn(pair(mn_s), w_up))
        d_up = split(dot_nt(pair(ct_s), pair(wd, cols)) * slope)
        hidden = split(hidden)
        blocks = FF // LANES
        grad = weight_grad(0, d_up)
        for j in range(FF_BLOCK // LANES):
            start = row_of[2] + f * (FF_BLOCK // LANES) + j
            grad_ref[pl.ds(start, D, stride=blocks), :] = grad[:, j * LANES : (j + 1) * LANES]
        grad = jnp.transpose(weight_grad(1, hidden))
        blocks = D // LANES
        for j in range(blocks):
            start = row_of[3] + f * (FF_BLOCK * blocks) + j
            grad_ref[pl.ds(start, FF_BLOCK, stride=blocks), :] = grad[:, j * LANES : (j + 1) * LANES]
        acc[...] += dot_nt(d_up, w_up)
        return carry

    lax.fori_loop(0, FF // FF_BLOCK, feed, 0)
    yield

    d_mixed = ct_ref[...] + normalize_backward(acc[...], full(mn_s), spread[1][:, :1])
    acc[...] = d_mixed
    d_pair = split(d_mixed)
    put_turned(0, ctx_s[...])
    grad = weight_grad(0, d_pair)
    blocks = D // LANES
    for j in range(blocks):
        grad_ref[pl.ds(row_of[1] + j, D, stride=blocks), :] = grad[:, j * LANES : (j + 1) * LANES]
    d_s[...] = dot_nt(d_pair, pair(wp))
    dbias[...] = jnp.zeros_like(dbias)
    yield
    tiles = D // LANES

    def backward(unit, carry):
        w, t = unit // tiles, unit % tiles
        rows = pl.ds(pl.multiple_of(w * TOK, TOK), TOK)
        cols = pl.ds(pl.multiple_of(t * LANES, LANES), LANES)
        k, v = tile(1, t, rows), tile(2, t, rows)
        grad = d_s[rows, cols]
        weighed = grad * ctx_s[rows, cols]
        g = split(grad)
        g_turned = split(jnp.transpose(grad))
        q_turned = split(jnp.transpose(q_s[rows, cols]))
        dq = jnp.zeros((TOK, LANES), F32)
        dk, dv = [], []
        for head in range(PACK):
            h = t * PACK + head
            part = slice(head * HEAD_DIM, (head + 1) * HEAD_DIM)
            upper, lower = prob[0, w * heads + h], prob[1, w * heads + h]
            dprob = dot_nt(only(head, g), v)
            delta = jnp.sum(jnp.where(lane_head == head, weighed, 0.0), axis=-1, keepdims=True)
            dscore = (upper.astype(F32) + lower.astype(F32)) * (dprob - delta)
            dbias[h] += dscore
            ds = split(dscore)
            dq += dot_cols(ds, only(head, k))
            dk.append(dot_rows((q_turned[0][part], q_turned[1][part]), ds))
            dv.append(dot_rows((g_turned[0][part], g_turned[1][part]), (upper, lower)))
        for j, value in enumerate((dq * SCALE, jnp.transpose(jnp.concatenate(dk, 0)),
                                   jnp.transpose(jnp.concatenate(dv, 0)))):
            at = pl.ds(pl.multiple_of(j * D + t * LANES, LANES), LANES)
            upper, lower = split(value)
            dqkv_s[0, rows, at], dqkv_s[1, rows, at] = upper, lower
        return carry

    for unit in range(0, count * tiles, SEGMENT):
        lax.fori_loop(unit, min(unit + SEGMENT, count * tiles), backward, 0)
        yield

    x_normed = full(xn_s)
    put_turned(1, x_normed)
    grad = weight_grad(1, pair(dqkv_s))
    blocks = 3 * D // LANES
    for j in range(blocks):
        grad_ref[pl.ds(row_of[0] + j, D, stride=blocks), :] = grad[:, j * LANES : (j + 1) * LANES]
    yield
    d_normed = dot_nt(pair(dqkv_s), pair(wq))
    yield
    q_s[...] = acc[...] + normalize_backward(d_normed, x_normed, spread[0][:, :1])
    edge_ref[...] = jnp.zeros_like(edge_ref)
    for at, row, col in window_pieces(height, breadth):
        edge_ref[row, col : col + WIN] = q_s[at : at + WIN]

    yield
    table_acc = jnp.zeros((levels * 2 * HEAD_ROWS, LANES), F32)

    def collect(block, total):
        rows = pl.ds(pl.multiple_of(block * 8, 8), 8)
        at_rows = index_ref[rows, :]
        grads = dbias[:, rows, :]
        for r in range(8):
            at = at_rows[r : r + 1]
            low, level_of = at & (LANES - 1), at >> 7
            grad = jnp.concatenate([grads[:, r, :], jnp.zeros((HEAD_ROWS - heads, TOK), F32)], 0)
            stacked = jnp.concatenate(
                [jnp.where(level_of == level, grad, 0.0) for level in range(levels)], 0)
            hot = (lax.broadcasted_iota(jnp.int32, (LANES, TOK), 0) == low).astype(F32).astype(BF16)
            total = total + mul(jnp.concatenate(split(stacked), 0), hot, NT)
        return total

    total = lax.fori_loop(0, TOK // 8, collect, table_acc)
    table_out[...] = total[: levels * HEAD_ROWS] + total[levels * HEAD_ROWS :]


def block_kernel(*refs):
    for _ in block_steps(*refs):
        pass


def block_scratch(tokens, height, breadth, heads, entries):
    levels = -(-entries // LANES)
    return [
        pltpu.VMEM((2, D, 3 * D), BF16),
        pltpu.VMEM((2, D, D), BF16),
        pltpu.VMEM((2, D, FF), BF16),
        pltpu.VMEM((2, FF, D), BF16),
        pltpu.VMEM((HEAD_ROWS, levels * LANES), F32),
        pltpu.VMEM((TOK, 2 * LANES), jnp.int32),
        pltpu.VMEM((heads, TOK, TOK), F32),
        pltpu.VMEM((2, tokens // TOK * heads, TOK, TOK), BF16),
        pltpu.VMEM((2, tokens, D), BF16),
        pltpu.VMEM((2, tokens, D), BF16),
        pltpu.VMEM((2, tokens, D), BF16),
        pltpu.VMEM((2, tokens, 3 * D), BF16),
        pltpu.VMEM((tokens, D), F32),
        pltpu.VMEM((tokens, D), F32),
        pltpu.VMEM((2, D, 3 * tokens), BF16),
        pltpu.VMEM((tokens, D), F32),
        pltpu.VMEM((height, breadth), F32),
        pltpu.VMEM((2, tokens, LANES), F32),
    ]


def table_rows(entries):
    return -(-entries // LANES) * HEAD_ROWS


def block_gradients(x, ct, weights, bias_table, bias_index, region_ids):
    tokens = x.shape[0]
    height, breadth = region_ids.shape
    heads, entries = bias_table.shape
    vmem = pl.BlockSpec(memory_space=pltpu.VMEM)
    return pl.pallas_call(
        block_kernel,
        in_specs=[vmem] * 6,
        out_specs=[vmem] * 3,
        out_shape=[
            jax.ShapeDtypeStruct((weights.shape[0] // LANES, LANES), F32),
            jax.ShapeDtypeStruct((height + SHIFT, breadth + EDGE, D), F32),
            jax.ShapeDtypeStruct((table_rows(entries), LANES), F32),
        ],
        scratch_shapes=[pltpu.VMEM((tokens, D), F32)]
        + block_scratch(tokens, height, breadth, heads, entries),
        compiler_params=pltpu.CompilerParams(vmem_limit_bytes=VMEM_LIMIT),
    )(x, ct, weights.reshape(-1, LANES), bias_table, bias_index, region_ids)


def bit_count(size):
    return size.bit_length() - 1


def bit_partners(lat_bits, lon_bits):
    bits = lat_bits + lon_bits
    lat, lon = lax.axis_index("lat"), lax.axis_index("lon")
    mine, partner = [], []
    for b in range(bits):
        if b < lat_bits:
            step = 1 << (lat_bits - 1 - b)
            bit = lax.rem(lat // step, 2)
            partner.append({"lat": lat + step * (1 - 2 * bit), "lon": lon})
        else:
            step = 1 << (bits - 1 - b)
            bit = lax.rem(lon // step, 2)
            partner.append({"lat": lat, "lon": lon + step * (1 - 2 * bit)})
        mine.append(bit)
    return mine, partner


class HalfExchange:
    def __init__(self, side, mine, partner, orders, chunks, factor, grad, held, own_weight, first_ref,
                 second_ref, new_ref, first_out, second_out, sems):
        self.side, self.mine, self.partner, self.orders = side, mine, partner, orders
        self.chunks, self.factor, self.grad, self.held = chunks, factor, grad, held
        self.own_weight, self.first_ref, self.second_ref = own_weight, first_ref, second_ref
        self.new_ref, self.first_out, self.second_out = new_ref, first_out, second_out
        self.sums, self.sent = sems[:2], sems[2:]
        self.owner, self.other = mine[0] == side, mine[0] != side
        self.bits = len(mine)

    def copy(self, src, dst, sems, i, s):
        return pltpu.make_async_remote_copy(
            src_ref=src, dst_ref=dst, send_sem=sems[0].at[self.side, i, s],
            recv_sem=sems[1].at[self.side, i, s], device_id=self.partner[self.orders[i][s]],
            device_id_type=pl.DeviceIdType.MESH)

    def run(self, owners_only, action):
        if owners_only:
            pl.when(self.owner)(action)
        else:
            action()

    def source(self, i, s, kept):
        b = self.orders[i][s]
        if b == 0:
            return self.held[i][s - 1], ()
        dims = sorted(d for d in self.orders[i][s:] if d)
        value = self.mine[b] if kept else 1 - self.mine[b]
        index = tuple(value if d == b else slice(None) for d in dims)
        if s == 0:
            return self.grad, (self.side,) + index + (pl.ds(*self.chunks[i]),)
        return self.held[i][s - 1], index

    def reduce_copy(self, i, s):
        ref, index = self.source(i, s, False)
        return self.copy(ref.at[index] if index else ref, self.held[i][s], self.sums, i, s)

    def reduce_start(self, i, s):
        def start():
            self.reduce_copy(i, s).start()

        if self.orders[i][s] == 0:
            pl.when(self.other)(start)
        else:
            self.run(0 in self.orders[i][:s], start)

    def reduce_finish(self, i, s):
        def add():
            ref, index = self.source(i, s, True)
            self.held[i][s][...] += ref[index] if index else ref[...]

        def both():
            self.reduce_copy(i, s).wait()
            add()

        def take():
            self.reduce_copy(i, s).wait_recv()
            add()

        def given():
            self.reduce_copy(i, s).wait_send()

        if self.orders[i][s] == 0:
            pl.when(self.other)(given)
            pl.when(self.owner)(take)
        else:
            self.run(0 in self.orders[i][:s], both)
        if s + 1 < self.bits:
            self.reduce_start(i, s + 1)
        else:
            pl.when(self.owner)(functools.partial(self.update, i))
            self.gather_start(i, s)

    def update(self, i):
        rows = pl.ds(*self.chunks[i])
        grad = self.held[i][self.bits - 1][...] * self.factor
        first = 0.9 * self.first_ref[rows] + 0.1 * grad
        second = 0.95 * self.second_ref[rows] + 0.05 * grad * grad
        self.first_out[rows] = first
        self.second_out[rows] = second
        self.new_ref[(self.side,) + tuple(self.mine[1:]) + (rows,)] = (
            self.own_weight[rows] - 0.01 * first / (jnp.sqrt(second) + 1e-08))

    def gather_copy(self, i, s):
        known = self.orders[i][s + 1 :]
        index = tuple(slice(None) if d in known else self.mine[d] for d in range(1, self.bits))
        region = self.new_ref.at[(self.side,) + index + (pl.ds(*self.chunks[i]),)]
        return self.copy(region, region, self.sent, i, s)

    def gather_start(self, i, s):
        def start():
            self.gather_copy(i, s).start()

        self.run(0 in self.orders[i][: s + 1], start)

    def gather_finish(self, i, s):
        def both():
            self.gather_copy(i, s).wait()

        def given():
            self.gather_copy(i, s).wait_send()

        def take():
            self.gather_copy(i, s).wait_recv()

        if self.orders[i][s] == 0:
            pl.when(self.owner)(given)
            pl.when(self.other)(take)
        else:
            self.run(0 in self.orders[i][:s], both)
        if s > 0:
            self.gather_start(i, s - 1)


class Edges:
    def __init__(self, edge_ref, dx_out, landing, sems):
        self.edge, self.out, self.landing, self.sems = edge_ref, dx_out, landing, sems

    def copies(self):
        height, breadth, _ = self.out.shape
        sources = (
            self.edge.at[pl.ds(SHIFT, height - SHIFT), pl.ds(breadth, EDGE)],
            self.edge.at[pl.ds(height, SHIFT), pl.ds(0, breadth)],
            self.edge.at[pl.ds(height, SHIFT), pl.ds(breadth, EDGE)],
        )
        return [
            pltpu.make_async_remote_copy(
                src_ref=src, dst_ref=dst, send_sem=self.sems[0].at[n], recv_sem=self.sems[1].at[n],
                device_id=where, device_id_type=pl.DeviceIdType.MESH)
            for n, (src, dst, where) in enumerate(zip(sources, self.landing, neighbours(1)))
        ]

    def start(self):
        for copy in self.copies():
            copy.start()

    def finish(self):
        for copy in self.copies():
            copy.wait()
        edge, out, (west, north, corner) = self.edge, self.out, self.landing
        height, breadth, _ = out.shape
        out[SHIFT:, EDGE:] = edge[SHIFT:height, EDGE:breadth]
        out[:SHIFT, EDGE:] = north[:, EDGE:]
        column = lax.broadcasted_iota(jnp.int32, (1, EDGE, D), 1)
        out[SHIFT:, :EDGE] = jnp.where(column < SHIFT, west[...], edge[SHIFT:height, :EDGE])
        out[:SHIFT, :EDGE] = jnp.where(column < SHIFT, corner[...], north[:, :EDGE])


class TableSum:
    def __init__(self, part, held, total, final, order, partner, factor, sems):
        self.part, self.held, self.total, self.final = part, held, total, final
        self.order, self.partner, self.factor, self.sems = order, partner, factor, sems

    def copy(self, s):
        return pltpu.make_async_remote_copy(
            src_ref=self.total if s else self.part, dst_ref=self.held.at[s],
            send_sem=self.sems[0].at[s], recv_sem=self.sems[1].at[s],
            device_id=self.partner[self.order[s]], device_id_type=pl.DeviceIdType.MESH)

    def start(self, s):
        self.copy(s).start()

    def finish(self, s):
        self.copy(s).wait()
        self.total[...] = (self.total if s else self.part)[...] + self.held[s]
        if s + 1 < len(self.order):
            self.start(s + 1)
            return
        heads, entries = self.final.shape
        for level in range(-(-entries // LANES)):
            width = min(LANES, entries - level * LANES)
            self.final[:, pl.ds(level * LANES, width)] = (
                self.total[pl.ds(level * HEAD_ROWS, heads), pl.ds(0, width)] * self.factor
            )


def exchange_parts(lat_bits, lon_bits, chunks, factor, grad, table_part, edge_ref, weight_ref, first_ref,
                   second_ref, new_ref, first_out, second_out, table_final, dx_out, *scratch):
    bits = lat_bits + lon_bits
    mine, partner = bit_partners(lat_bits, lon_bits)
    core, inner, ahead = bits - 1, list(range(lat_bits, bits - 1))[::-1], list(range(lat_bits))[::-1]
    orders = [[core] + (inner + ahead if i % 2 else ahead + inner) for i in range(len(chunks))]
    held = [scratch[i * bits : (i + 1) * bits] for i in range(2 * len(chunks))]
    table_held, table_total, *landing, own_weight = scratch[2 * len(chunks) * bits :][:6]
    sems = scratch[2 * len(chunks) * bits + 6 :]
    fetch = pltpu.make_async_copy(weight_ref.at[tuple(mine)], own_weight, sems[8])
    fetch.start()
    halves = [
        HalfExchange(side, mine, partner, orders, chunks, factor, grad,
                     held[side * len(chunks) : (side + 1) * len(chunks)], own_weight, first_ref,
                     second_ref, new_ref, first_out, second_out, sems[:4])
        for side in range(2)
    ]
    table = TableSum(table_part, table_held, table_total, table_final, orders[0], partner, factor, sems[4:6])
    return fetch, halves, Edges(edge_ref, dx_out, landing, sems[6:8]), table


def exchange_kernel(lat_bits, lon_bits, chunks, factor, *refs):
    greet(bit_partners(lat_bits, lon_bits)[1] + list(neighbours(-1)))
    fetch, (low, high), edges, table = exchange_parts(lat_bits, lon_bits, chunks, factor, *refs)
    each, bits = range(len(chunks)), lat_bits + lon_bits
    for half in (high, low):
        for i in each:
            half.reduce_start(i, 0)
    edges.start()
    table.start(0)
    fetch.wait()
    for s in range(bits):
        for half in (high, low):
            for i in each:
                half.reduce_finish(i, s)
        table.finish(s)
    edges.finish()
    for s in reversed(range(bits)):
        for half in (high, low):
            for i in each:
                half.gather_finish(i, s)


def chunk_rows(rows, count):
    groups = -(-rows // 8)
    edges = [min(8 * (groups * i // count), rows) for i in range(count)] + [rows]
    return [(a, b - a) for a, b in zip(edges, edges[1:])]


def exchange_scratch(bits, chunks, rows, table_shape, tile_shape):
    height, breadth, _ = tile_shape
    dma = pltpu.SemaphoreType.DMA
    lat_bits = bit_count(lax.axis_size("lat"))

    def left(i, s):
        first_at = bits - 1 if i % 2 else lat_bits
        return bits - 2 - s + (1 if s >= first_at else 0)

    return [
        pltpu.VMEM((2,) * left(i, s) + (chunks[i][1], LANES), F32)
        for _ in range(2)
        for i in range(len(chunks))
        for s in range(bits)
    ] + [
        pltpu.VMEM((bits,) + table_shape, F32),
        pltpu.VMEM(table_shape, F32),
        pltpu.VMEM((height - SHIFT, EDGE, D), F32),
        pltpu.VMEM((SHIFT, breadth, D), F32),
        pltpu.VMEM((SHIFT, EDGE, D), F32),
        pltpu.VMEM((rows, LANES), F32),
    ] + [dma((2, len(chunks), bits))] * 4 + [dma((bits,))] * 2 + [dma((3,))] * 2 + [dma(())]


def fused_kernel(lat_bits, lon_bits, chunks, factor, n_exchange, x_hbm, ct_hbm, weight_ref, table_ref,
                 index_ref, region_ref, first_ref, second_ref, new_ref, first_out, second_out,
                 table_final, dx_out, grad, table_part, xw, ctw, wide, send, recv, local, w_sem, *scratch):
    greet(bit_partners(lat_bits, lon_bits)[1] + list(neighbours(1)) + list(neighbours(-1)))
    staged = pltpu.make_async_copy(weight_ref, new_ref, w_sem)
    staged.start()
    copies = [halo_copies(n, ref, wide, send, recv, local) for n, ref in enumerate((x_hbm, ct_hbm))]
    edge = wide.at[0]
    block = block_steps(xw, ctw, new_ref.reshape(grad.shape), table_ref, index_ref, region_ref, grad,
                        edge, table_part, xw, *scratch[n_exchange:])
    fetch, (low, high), edges, table = exchange_parts(
        lat_bits, lon_bits, chunks, factor, grad.reshape(new_ref.shape), table_part, edge, weight_ref,
        first_ref, second_ref, new_ref, first_out, second_out, table_final, dx_out, *scratch[:n_exchange])
    each, bits = range(len(chunks)), lat_bits + lon_bits
    waiting = [(s, i) for s in range(1, bits) for i in each]

    def advance(count):
        for s, i in waiting[:count]:
            high.reduce_finish(i, s)
        del waiting[:count]

    next(block)
    staged.wait()
    next(block)
    assemble(0, copies[0], x_hbm.shape, wide, xw)
    next(block)
    assemble(1, copies[1], x_hbm.shape, wide, ctw)
    next(block)
    for i in each:
        high.reduce_start(i, 0)
    next(block)
    for i in each:
        high.reduce_finish(i, 0)
    fetch.wait()
    units = region_ref.size // TOK * (D // LANES)
    for n in range(-(-units // SEGMENT)):
        next(block)
        advance(PACE[n] if n < len(PACE) else 0)
    next(block)
    for i in each:
        low.reduce_start(i, 0)
    advance(LATER[0])
    next(block)
    for i in each:
        low.reduce_finish(i, 0)
    advance(LATER[1])
    next(block)
    edges.start()
    advance(len(waiting))
    for _ in block:
        pass
    table.start(0)
    for s in range(1, bits):
        for i in each:
            low.reduce_finish(i, s)
        for i in each:
            high.gather_finish(i, bits - s)
        table.finish(s - 1)
    for i in each:
        high.gather_finish(i, 0)
    table.finish(bits - 1)
    edges.finish()
    for s in reversed(range(bits)):
        for i in each:
            low.gather_finish(i, s)


def whole_step(block_input, cotangent, weights, first, second, bias_table, bias_index, region_ids, factor):
    lat_bits, lon_bits = bit_count(lax.axis_size("lat")), bit_count(lax.axis_size("lon"))
    bits = lat_bits + lon_bits
    rows = first.shape[0] // LANES
    chunks = chunk_rows(rows, CHUNKS)
    split_shape = (2,) * bits + (rows, LANES)
    tile_shape = block_input.shape
    height, breadth, _ = tile_shape
    tokens = height * breadth
    heads, entries = bias_table.shape
    table_shape = (table_rows(entries), LANES)
    vmem, anywhere = pl.BlockSpec(memory_space=pltpu.VMEM), pl.BlockSpec(memory_space=pl.ANY)
    shard = jax.ShapeDtypeStruct((rows, LANES), F32)
    dma = pltpu.SemaphoreType.DMA
    for_exchange = exchange_scratch(bits, chunks, rows, table_shape, tile_shape)
    new, first_new, second_new, table_sum, dx = pl.pallas_call(
        functools.partial(fused_kernel, lat_bits, lon_bits, chunks, factor, len(for_exchange)),
        in_specs=[anywhere] * 3 + [vmem] * 5,
        out_specs=[vmem] * 5,
        out_shape=[jax.ShapeDtypeStruct(split_shape, F32), shard, shard,
                   jax.ShapeDtypeStruct(bias_table.shape, F32),
                   jax.ShapeDtypeStruct(tile_shape, F32)],
        scratch_shapes=[
            pltpu.VMEM((weights.shape[0] // LANES, LANES), F32),
            pltpu.VMEM(table_shape, F32),
            pltpu.VMEM((tokens, D), F32),
            pltpu.VMEM((tokens, D), F32),
            pltpu.VMEM((2, height + SHIFT, breadth + EDGE, D), F32),
            dma((2, 3)), dma((2, 3)), dma((2,)), dma(()),
        ] + for_exchange + block_scratch(tokens, height, breadth, heads, entries),
        compiler_params=pltpu.CompilerParams(
            collective_id=2, has_side_effects=True, vmem_limit_bytes=VMEM_LIMIT),
    )(block_input, cotangent, weights.reshape(split_shape), bias_table, bias_index, region_ids,
      first.reshape(rows, LANES), second.reshape(rows, LANES))
    return new.reshape(-1), first_new.reshape(-1), second_new.reshape(-1), table_sum, dx


def reduce_update_gather(grads, table, edge, weights, first, second, table_shape, tile_shape, factor):
    lat_bits, lon_bits = bit_count(lax.axis_size("lat")), bit_count(lax.axis_size("lon"))
    bits = lat_bits + lon_bits
    rows = first.shape[0] // LANES
    chunks = chunk_rows(rows, CHUNKS)
    split_shape = (2,) * bits + (rows, LANES)
    vmem = pl.BlockSpec(memory_space=pltpu.VMEM)
    shard = jax.ShapeDtypeStruct((rows, LANES), F32)
    new, first_new, second_new, table_sum, dx = pl.pallas_call(
        functools.partial(exchange_kernel, lat_bits, lon_bits, chunks, factor),
        in_specs=[vmem, vmem, vmem, pl.BlockSpec(memory_space=pl.ANY), vmem, vmem],
        out_specs=[vmem] * 5,
        out_shape=[jax.ShapeDtypeStruct(split_shape, F32), shard, shard,
                   jax.ShapeDtypeStruct(table_shape, F32),
                   jax.ShapeDtypeStruct(tile_shape, F32)],
        scratch_shapes=exchange_scratch(bits, chunks, rows, table.shape, tile_shape),
        compiler_params=pltpu.CompilerParams(
            collective_id=0, has_side_effects=True, vmem_limit_bytes=56 * 1024 * 1024),
    )(grads.reshape(split_shape), table, edge, weights.reshape(split_shape),
      first.reshape(rows, LANES), second.reshape(rows, LANES))
    return new.reshape(-1), first_new.reshape(-1), second_new.reshape(-1), table_sum, dx


def per_device(
    block_input, cotangent, weights, first_moment, second_moment, bias_table, bias_index, region_ids
):
    tile_rows, tile_cols, _ = block_input.shape
    devices = lax.axis_size("lat") * lax.axis_size("lon")
    factor = 1.0 / math.sqrt(tile_rows * tile_cols * devices)
    if first_moment.shape[0] % (8 * LANES) == 0:
        gathered, first_new, second_new, table_grad, grad_input = whole_step(
            block_input, cotangent, weights, first_moment, second_moment, bias_table, bias_index,
            region_ids, factor,
        )
        return (grad_input, gathered, first_new, second_new, table_grad)
    x, ct = gather_windows(block_input, cotangent)
    grads, edge, table = block_gradients(x, ct, weights, bias_table, bias_index, region_ids)
    gathered, first_new, second_new, table_grad, grad_input = reduce_update_gather(
        grads, table, edge, weights, first_moment, second_moment, bias_table.shape,
        block_input.shape, factor,
    )
    return (grad_input, gathered, first_new, second_new, table_grad)


def solution(mesh):
    placed = (
        P("lat", "lon", None),
        P("lat", "lon", None),
        P(),
        P(("lat", "lon")),
        P(("lat", "lon")),
        P(),
        P(),
        P("lat", "lon"),
    )
    return jax.shard_map(
        per_device,
        mesh=mesh,
        in_specs=placed,
        out_specs=(P("lat", "lon", None), P(), P(("lat", "lon")), P(("lat", "lon")), P()),
        check_vma=False,
    )
```
